512 devices in a mesh: row: 32 (over z_lo, x), col: 16 (over z_hi, y, core).
Axes of the slice: x: 4, y: 4, z: 16 (z_hi: 2, z_lo: 8; z = z_hi * 8 + z_lo), core: 2. Of those that a mesh axis runs over, the one named last changes fastest.
Arguments:
- noisy: float32 [1024, 32768], P('row', 'col'), may hold values from -9 to 9
Outputs:
- denoised: float32 [1024, 32768], P('row', 'col')
- gap: float32 [4], replicated
The draws below stay inside these ranges and needn't reach their ends.
All inputs are finite; a program needn't handle non-finite values.
Results may differ from the reference program's by a relative error of at most 0.0003.
Values sent between devices are 32-bit elements; how exact they have to be, the bound alone decides.
A program may use at most 64 MiB of HBM per device.

```python
import jax
import jax.numpy as jnp

ITERS = 4
H = 1024
W = 32768


def draw_noisy(key, part):
    first, second = jax.random.split(jax.random.fold_in(key, 17), 2)
    levels = jax.random.uniform(first, (H // 16 + 1, W // 16 + 1), jnp.float32, -1.0, 1.0)
    blocky = jnp.repeat(jnp.repeat(levels, 16, axis=0), 16, axis=1)[:H, :W]
    grain = jnp.clip(jax.random.normal(second, (H, W), jnp.float32), -3.0, 3.0) * 0.6
    row_scale = jnp.exp(jnp.log(3.0) * jnp.arange(H, dtype=jnp.float32) / (H - 1))
    return row_scale[:, None] * (blocky + grain)


def setup_inputs(seed: int = 0) -> dict:
    streams_of = jax.random.split(jax.random.key(seed), 2)
    return {
        "noisy": draw_noisy(jax.random.fold_in(streams_of[1], 71), 0),
    }


fidelity = 8.0
primal_step = 0.35
dual_step = 0.35

def forward_grads(field):
    row_count, col_count = field.shape
    row_diff = jnp.concatenate([field[1:] - field[:-1], jnp.zeros((1, col_count), jnp.float32)], 0)
    col_diff = jnp.concatenate([field[:, 1:] - field[:, :-1], jnp.zeros((row_count, 1), jnp.float32)], 1)
    return (row_diff, col_diff)

def divergence(dual_rows, dual_cols):
    row_count, col_count = dual_rows.shape
    shifted_rows = jnp.concatenate([jnp.zeros((1, col_count), jnp.float32), dual_rows[:-1]], 0)
    shifted_cols = jnp.concatenate([jnp.zeros((row_count, 1), jnp.float32), dual_cols[:, :-1]], 1)
    return dual_rows - shifted_rows + dual_cols - shifted_cols

def reference(noisy):
    primal = noisy
    previous = noisy
    dual_rows = jnp.zeros_like(noisy)
    dual_cols = jnp.zeros_like(noisy)
    gaps = []
    for iteration in range(ITERS):
        extrapolated = 2.0 * primal - previous
        grad_rows, grad_cols = forward_grads(extrapolated)
        trial_rows = dual_rows + dual_step * grad_rows
        trial_cols = dual_cols + dual_step * grad_cols
        shrink = 1.0 / jnp.maximum(1.0, jnp.sqrt(trial_rows * trial_rows + trial_cols * trial_cols))
        dual_rows = trial_rows * shrink
        dual_cols = trial_cols * shrink
        diverged = divergence(dual_rows, dual_cols)
        updated = (primal + primal_step * diverged + primal_step * fidelity * noisy) / (1.0 + primal_step * fidelity)
        previous = primal
        primal = updated
        edge_rows, edge_cols = forward_grads(primal)
        total = jnp.sum(jnp.sqrt(edge_rows * edge_rows + edge_cols * edge_cols)) + jnp.sum(0.5 * fidelity * (primal - noisy) ** 2 + noisy * diverged + diverged * diverged / (2.0 * fidelity))
        gaps.append(total / (H * W))
    return (primal, jnp.stack(gaps))
```

```python
import jax
import jax.numpy as jnp
from jax import lax
from jax.experimental import pallas as pl
from jax.experimental.pallas import tpu as pltpu
from jax.sharding import PartitionSpec as P

ITERS = 4
Z_LO, X, Z_HI, Y = 8, 4, 2, 4
Z = Z_HI * Z_LO
N_ROW, N_COL = Z_LO * X, Z_HI * Y * 2
ROOTS = X * Y
TR, TC = 32, 2048
NT = TC // 128
FR = 40
BASE = 8
BUF = 56
TOP = 4
STRIP = NT
EDGE = 8

FIDELITY = 8.0
PSTEP = 0.35
DSTEP = 0.35
KA = 1.0 / (1.0 + PSTEP * FIDELITY)
KB = PSTEP / (1.0 + PSTEP * FIDELITY)
KC = PSTEP * FIDELITY / (1.0 + PSTEP * FIDELITY)
CELLS = float(N_ROW * TR * N_COL * TC)
TINY = 1e-37

SIDES = [(dr, dc) for dr in (-1, 0, 1) for dc in (-1, 0, 1) if (dr, dc) != (0, 0)]


def kernel(
    noisy, out, gap, own, top, bot, lef, rig, corners, nf, nc, xs, pr, pc, er, ec, gr, gc,
    msg, part, plane, result, own_sem, send_sem, recv_sem, part_send, part_recv, plane_send, plane_recv,
    result_send, result_recv,
):
    f32 = jnp.float32
    row, col = lax.axis_index("row"), lax.axis_index("col")
    zl, x = row // X, row % X
    zh, y, core = col // (2 * Y), (col // 2) % Y, col % 2
    z = zh * Z_LO + zl
    lane = lax.broadcasted_iota(jnp.int32, (FR, 128), 1)
    sub = lax.broadcasted_iota(jnp.int32, (FR, 128), 0)
    is_root = (z == 0) & (core == 1)
    early = col == 2 * Y - 1
    late = col == 2 * Y

    def ident(r, c):
        return r * N_COL + c

    def exists(dr, dc):
        cond = None
        for t in ([row >= 1] if dr < 0 else [row < N_ROW - 1] if dr > 0 else []) + (
            [col >= 1] if dc < 0 else [col < N_COL - 1] if dc > 0 else []
        ):
            cond = t if cond is None else cond & t
        return cond

    root_id = ident(x, y * 2 + 1)
    own_copy = pltpu.make_async_copy(noisy, own, own_sem)
    own_copy.start()

    barrier = pltpu.get_barrier_semaphore()

    def signal(target):
        pl.semaphore_signal(barrier, inc=1, device_id=target, device_id_type=pl.DeviceIdType.LOGICAL)

    heard = []
    for dr, dc in SIDES:
        greet = exists(dr, dc)
        if dc < 0:
            greet = greet & jnp.logical_not(late)
        pl.when(greet)(lambda dr=dr, dc=dc: signal(ident(row + dr, col + dc)))
        hear = exists(dr, dc)
        if dc > 0:
            hear = hear & jnp.logical_not(early)
        heard.append(hear)

    @pl.when(is_root)
    def _():
        for i in range(ROOTS):
            xx, yy = i // Y, i % Y

            @pl.when((x != xx) | (y != yy))
            def _():
                signal(ident(xx, yy * 2 + 1))

        signal(ident(row, col - 1))

        @pl.loop(1, Z)
        def _(zz):
            r, c = lax.rem(zz, Z_LO) * X + x, ((zz // Z_LO) * Y + y) * 2
            signal(ident(r, c))
            signal(ident(r, c + 1))


    for cond, buf in ((row == 0, top), (row == N_ROW - 1, bot), (col == 0, lef), (col == N_COL - 1, rig)):

        @pl.when(cond)
        def _():
            buf[...] = jnp.zeros_like(buf)

    for i, (dr, dc) in enumerate([(-1, -1), (-1, 1), (1, -1), (1, 1)]):

        @pl.when(jnp.logical_not(exists(dr, dc)))
        def _():
            corners[i] = jnp.zeros((8, 128), f32)

    for ref in (xs, pr):
        for t in range(NT + 1):
            ref[t, 0:BASE, :] = jnp.zeros((BASE, 128), f32)
            ref[t, BASE + FR : BUF, :] = jnp.zeros((BUF - BASE - FR, 128), f32)

    own_copy.wait()
    count = jnp.where(is_root, ROOTS - 1, 1)
    for hear in heard:
        count = count + jnp.where(hear, 1, 0)
    pl.semaphore_wait(barrier, count)

    place = {
        (-1, 0): top, (1, 0): bot, (0, -1): lef, (0, 1): rig, (-1, -1): corners.at[0], (-1, 1): corners.at[1],
        (1, -1): corners.at[2], (1, 1): corners.at[3],
    }

    def source(dr, dc):
        rs = slice(0, TR) if dr == 0 else slice(0, 8) if dr < 0 else slice(TR - 8, TR)
        cs = slice(0, TC) if dc == 0 else slice(0, 128) if dc < 0 else slice(TC - 128, TC)
        return own.at[rs, cs]

    def halo(dr, dc):
        i = SIDES.index((dr, dc))
        return pltpu.make_async_remote_copy(
            source(dr, dc), place[(-dr, -dc)], send_sem.at[i], recv_sem.at[SIDES.index((-dr, -dc))],
            device_id=ident(row + dr, col + dc), device_id_type=pl.DeviceIdType.LOGICAL,
        )

    def arrived(dr, dc):
        i = SIDES.index((dr, dc))
        return pltpu.make_async_remote_copy(
            source(-dr, -dc), place[(dr, dc)], send_sem.at[i], recv_sem.at[i],
            device_id=ident(row, col), device_id_type=pl.DeviceIdType.LOGICAL,
        )

    for dr, dc in [(1, 0), (-1, 0), (0, 1), (0, -1), (1, 1), (1, -1), (-1, 1), (-1, -1)]:
        cond = exists(dr, dc)
        if dc > 0:
            cond = cond & jnp.logical_not(early)
        pl.when(cond)(lambda dr=dr, dc=dc: halo(dr, dc).start())

    grow = row * TR - TOP + sub
    row_mask = jnp.where((grow >= 0) & (grow < N_ROW * TR - 1), DSTEP, 0.0).astype(f32)
    rows_in = (sub >= TOP) & (sub < TOP + TR)

    def frame(ref, t, shift=0):
        return ref[t, BASE + shift : BASE + shift + FR, :]

    def left_of(v):
        return pltpu.roll(v, 1, 1)

    def right_of(v):
        return pltpu.roll(v, 127, 1)

    def sums(cell):
        acc = cell[0:8]
        for i in range(1, FR // 8):
            acc = acc + cell[8 * i : 8 * i + 8]
        return acc

    def sweeps(tiles, col_mask, keep):
        acc_a, acc_b = [], []
        for k in range(ITERS):
            a_sum = b_sum = None
            prev_pc = None
            pend = None
            rolled_n = None
            for t in tiles + [None]:
                if t is not None:
                    n = frame(nf, t)
                    if k == 0:
                        ncol = right_of(n) if rolled_n is None else rolled_n
                        if t != tiles[-1]:
                            rolled_n = right_of(frame(nf, t + 1))
                            nright = jnp.where(lane == 127, rolled_n, ncol)
                        else:
                            nright = ncol
                        qr = (frame(nf, t, 1) - n) * row_mask
                        qc = (nright - n) * col_mask
                        gr[t] = qr
                        gc[t] = qc
                    else:
                        qr = frame(pr, t) + er[t]
                        qc = pc[t] + ec[t]
                    shrink = lax.rsqrt(jnp.maximum(qr * qr + qc * qc, 1.0))
                    p_r = qr * shrink
                    p_c = qc * shrink
                    pr[t, BASE : BASE + FR, :] = p_r
                    if k < ITERS - 1:
                        pc[t] = p_c
                    rolled = left_of(p_c)
                    pleft = rolled if prev_pc is None else jnp.where(lane == 0, prev_pc, rolled)
                    prev_pc = rolled
                    d = (p_r - frame(pr, t, -1)) + (p_c - pleft)
                    if k == 0:
                        new = n + KB * d
                        nc[t] = n * KC
                    else:
                        new = KA * frame(xs, t) + (KB * d + nc[t])
                    xs[t, BASE : BASE + FR, :] = new
                    rolled_x = right_of(new)
                if pend is not None:
                    s, sx, sd, sn, srolled = pend
                    xright = srolled if t is None else jnp.where(lane == 127, rolled_x, srolled)
                    g_r = (frame(xs, s, 1) - sx) * row_mask
                    g_c = (xright - sx) * col_mask
                    if k < ITERS - 1:
                        er[s] = g_r + (g_r - gr[s])
                        ec[s] = g_c + (g_c - gc[s])
                        gr[s] = g_r
                        gc[s] = g_c
                    m = g_r * g_r + g_c * g_c
                    size = m * lax.rsqrt(jnp.maximum(m, TINY))
                    diff = sx - sn
                    rest = (diff * diff) * (0.5 * FIDELITY) + sd * (sn + sd * (0.5 / FIDELITY))
                    mask = keep(s)
                    size = sums(jnp.where(mask, size, 0.0))
                    rest = sums(jnp.where(mask, rest, 0.0))
                    a_sum = size if a_sum is None else a_sum + size
                    b_sum = rest if b_sum is None else b_sum + rest
                if t is not None:
                    pend = (t, new, d, n, rolled_x)
            acc_a.append(a_sum)
            acc_b.append(b_sum)
        return acc_a, acc_b

    def wait_side(dr, dc, extra=None):
        cond = exists(dr, dc)
        if extra is not None:
            cond = cond & extra
        pl.when(cond)(lambda: arrived(dr, dc).wait_recv())

    wait_side(-1, 0)
    wait_side(1, 0)
    for t in range(NT):
        cs = slice(128 * t, 128 * t + 128)
        nf[t, BASE + TOP - 8 : BASE + TOP, :] = top[:, cs]
        nf[t, BASE + TOP : BASE + TOP + TR, :] = own[:, cs]
        nf[t, BASE + TOP + TR : BASE + TOP + TR + 8, :] = bot[:, cs]

    def keep_main(t):
        if t == 0:
            return rows_in & (lane >= EDGE)
        if t == NT - 1:
            return rows_in & (lane < 128 - EDGE)
        return rows_in

    acc_a, acc_b = sweeps(list(range(NT)), DSTEP, keep_main)

    for dr in (-1, 0, 1):
        wait_side(dr, -1, jnp.logical_not(late))
        wait_side(dr, 1)

    for dr in (-1, 0, 1):
        pl.when(exists(dr, 1) & early)(lambda dr=dr: halo(dr, 1).start())

    def pack(last, right, left, first):
        q = lax.broadcasted_iota(jnp.int32, last.shape, 1)
        v = jnp.where(q < 32, pltpu.roll(last, 32, 1), pltpu.roll(right, 32, 1))
        w = jnp.where(q < 96, pltpu.roll(left, 96, 1), pltpu.roll(first, 96, 1))
        return jnp.where(q < 64, v, w)

    def strip_frame(with_left):
        def part_of(ref, i=None):
            return ref[...] if i is None else ref[i]

        def left_part(ref, i, like):
            return part_of(ref, i) if with_left else jnp.zeros_like(like)

        lo, hi = slice(0, 128), slice(TC - 128, TC)
        t_right, m_right, b_right = corners[1], rig[...], corners[3]
        nf[STRIP, BASE + TOP - 8 : BASE + TOP, :] = pack(top[:, hi], t_right, left_part(corners, 0, t_right), top[:, lo])
        nf[STRIP, BASE + TOP : BASE + TOP + TR, :] = pack(own[:, hi], m_right, left_part(lef, None, m_right), own[:, lo])
        nf[STRIP, BASE + TOP + TR : BASE + TOP + TR + 8, :] = pack(bot[:, hi], b_right, left_part(corners, 2, b_right), bot[:, lo])

    pl.when(late)(lambda: strip_frame(False))
    pl.when(jnp.logical_not(late))(lambda: strip_frame(True))
    outside = ((col == 0) & (lane >= 64) & (lane < 96)) | ((col == N_COL - 1) & (lane >= 31) & (lane < 64))
    strip_mask = jnp.where(outside, 0.0, DSTEP).astype(f32)
    owned = ((lane >= 32 - EDGE) & (lane < 32)) | (early & (lane >= 32) & (lane < 32 + EDGE))
    owned = owned | (jnp.logical_not(late) & (lane >= 96) & (lane < 96 + EDGE))
    owned = owned & rows_in
    strip_a, strip_b = sweeps([STRIP], strip_mask, lambda t: owned)

    lane8 = lax.broadcasted_iota(jnp.int32, (8, 128), 1)
    sub8 = lax.broadcasted_iota(jnp.int32, (8, 128), 0)
    table = jnp.zeros((8, 128), f32)
    for k in range(ITERS):
        total = (acc_a[k] + strip_a[k]) * (1.0 / DSTEP) + (acc_b[k] + strip_b[k])
        table = jnp.where(sub8 == k, jnp.sum(total, axis=0, keepdims=True), table)
    line = jnp.sum(table, axis=1, keepdims=True)
    line = jnp.sum(jnp.where(lane8 == sub8, line, 0.0), axis=0, keepdims=True)
    msg[...] = line

    slot = z * 2 + core
    part_copy = pltpu.make_async_remote_copy(
        msg, part.at[slot], part_send, part_recv, device_id=root_id, device_id_type=pl.DeviceIdType.LOGICAL
    )
    pl.when(jnp.logical_not(is_root))(lambda: part_copy.start())

    lane32 = lax.broadcasted_iota(jnp.int32, (TR, 128), 1)
    for t in range(NT):
        v = xs[t, BASE + TOP : BASE + TOP + TR, :]
        if t in (0, NT - 1):
            s = xs[STRIP, BASE + TOP : BASE + TOP + TR, :]
            if t == 0:
                v = jnp.where(lane32 < EDGE, pltpu.roll(s, 32, 1), v)
            else:
                v = jnp.where(lane32 >= 128 - EDGE, pltpu.roll(s, 96, 1), v)
        out[:, 128 * t : 128 * t + 128] = v

    @pl.when(late)
    def _():
        for dr in (-1, 0, 1):
            wait_side(dr, -1)
        strip_frame(True)
        sweeps([STRIP], strip_mask, lambda t: owned)
        s = xs[STRIP, BASE + TOP : BASE + TOP + TR, :]
        out[:, 0:128] = jnp.where(lane32 < EDGE, pltpu.roll(s, 32, 1), out[:, 0:128])

    def rows_of(ref, n, sem):
        return pltpu.make_async_copy(ref.at[0:n], ref.at[0:n], sem)

    @pl.when(is_root)
    def _():
        rows_of(part, 2 * Z - 1, part_recv).wait()
        part[1] = msg[...]
        total = part[0]
        for i in range(1, 2 * Z):
            total = total + part[i]
        me = x * Y + y
        plane[me] = total
        for i in range(ROOTS):
            xx, yy = i // Y, i % Y

            @pl.when((x != xx) | (y != yy))
            def _():
                pltpu.make_async_remote_copy(
                    plane.at[me], plane.at[me], plane_send, plane_recv,
                    device_id=ident(xx, yy * 2 + 1), device_id_type=pl.DeviceIdType.LOGICAL,
                ).start()

        rows_of(plane, ROOTS - 1, plane_recv).wait()
        total = plane[0]
        for i in range(1, ROOTS):
            total = total + plane[i]
        result[...] = total * (1.0 / CELLS)

        def tell(target):
            pltpu.make_async_remote_copy(
                result, result, result_send, result_recv, device_id=target, device_id_type=pl.DeviceIdType.LOGICAL
            ).start()

        tell(ident(row, col - 1))

        @pl.loop(1, Z)
        def _(zz):
            r, c = lax.rem(zz, Z_LO) * X + x, ((zz // Z_LO) * Y + y) * 2
            tell(ident(r, c))
            tell(ident(r, c + 1))

        gap[...] = result[...]
        rows_of(plane, ROOTS - 1, plane_send).wait()
        rows_of(part, 2 * Z - 1, result_send).wait()

    @pl.when(jnp.logical_not(is_root))
    def _():
        pltpu.make_async_copy(result, result, result_recv).wait()
        gap[...] = result[...]
        part_copy.wait_send()

    for dr, dc in SIDES:
        pl.when(exists(dr, dc))(lambda dr=dr, dc=dc: halo(dr, dc).wait_send())


def on_device(noisy):
    f32 = jnp.float32
    vmem = pl.BlockSpec(memory_space=pltpu.VMEM)
    frame = lambda rows: pltpu.VMEM((NT + 1, rows, 128), f32)
    dma = pltpu.SemaphoreType.DMA
    denoised, gap = pl.pallas_call(
        kernel,
        out_shape=(jax.ShapeDtypeStruct((TR, TC), f32), jax.ShapeDtypeStruct((1, 128), f32)),
        in_specs=[pl.BlockSpec(memory_space=pltpu.HBM)],
        out_specs=(vmem, vmem),
        scratch_shapes=[
            pltpu.VMEM((TR, TC), f32),
            pltpu.VMEM((8, TC), f32),
            pltpu.VMEM((8, TC), f32),
            pltpu.VMEM((TR, 128), f32),
            pltpu.VMEM((TR, 128), f32),
            pltpu.VMEM((4, 8, 128), f32),
            frame(BUF), frame(FR), frame(BUF), frame(BUF), frame(FR), frame(FR), frame(FR), frame(FR), frame(FR),
            pltpu.VMEM((1, 128), f32),
            pltpu.VMEM((2 * Z, 1, 128), f32),
            pltpu.VMEM((ROOTS, 1, 128), f32),
            pltpu.VMEM((1, 128), f32),
            dma, dma((8,)), dma((8,)), dma, dma, dma, dma, dma, dma,
        ],
        compiler_params=pltpu.CompilerParams(
            collective_id=0, has_side_effects=True, vmem_limit_bytes=16 * 1024 * 1024
        ),
    )(noisy)
    return denoised, gap[0, :ITERS]


def solution(mesh):
    return jax.shard_map(
        on_device,
        mesh=mesh,
        in_specs=(P("row", "col"),),
        out_specs=(P("row", "col"), P()),
        check_vma=False,
    )
```

```python
import jax
import jax.numpy as jnp
from jax import lax
from jax.experimental import pallas as pl
from jax.experimental.pallas import tpu as pltpu
from jax.sharding import PartitionSpec as P

ITERS = 4
Z_LO, X, Z_HI, Y = 8, 4, 2, 4
Z = Z_HI * Z_LO
N_ROW, N_COL = Z_LO * X, Z_HI * Y * 2
ROOTS = X * Y
TR, TC = 32, 2048
NT = TC // 128
FR = 40
BASE = 8
BUF = 56
TOP = 4
STRIP = NT
SEAM = NT + 1
EDGE = 8

FIDELITY = 8.0
PSTEP = 0.35
DSTEP = 0.35
KA = 1.0 / (1.0 + PSTEP * FIDELITY)
KB = PSTEP / (1.0 + PSTEP * FIDELITY)
KC = PSTEP * FIDELITY / (1.0 + PSTEP * FIDELITY)
CELLS = float(N_ROW * TR * N_COL * TC)
TINY = 1e-37

SIDES = [(dr, dc) for dr in (-1, 0, 1) for dc in (-1, 0, 1) if (dr, dc) != (0, 0)]


def kernel(
    noisy, out, gap, own, top, bot, lef, rig, corners, seam_mid, seam_up, seam_down, seam_out, seam_in, nf, nc, xs, pr, pc, er, ec, gr, gc,
    msg, part, plane, result, own_sem, send_sem, recv_sem, part_send, part_recv, plane_send, plane_recv,
    result_send, result_recv, seam_send, seam_recv, back_send, back_recv,
):
    f32 = jnp.float32
    row, col = lax.axis_index("row"), lax.axis_index("col")
    zl, x = row // X, row % X
    zh, y, core = col // (2 * Y), (col // 2) % Y, col % 2
    z = zh * Z_LO + zl
    lane = lax.broadcasted_iota(jnp.int32, (FR, 128), 1)
    sub = lax.broadcasted_iota(jnp.int32, (FR, 128), 0)
    is_root = (z == 0) & (core == 1)
    before, after = col == 2 * Y - 1, col == 2 * Y
    hub = z == 0
    hub_row = col * X + x

    def ident(r, c):
        return r * N_COL + c

    def hub_of(r):
        return ident(r % X, r // X)

    def exists(dr, dc):
        cond = jnp.logical_not(before if dc > 0 else after) if dc else None
        for t in ([row >= 1] if dr < 0 else [row < N_ROW - 1] if dr > 0 else []) + (
            [col >= 1] if dc < 0 else [col < N_COL - 1] if dc > 0 else []
        ):
            cond = t if cond is None else cond & t
        return cond

    root_id = ident(x, y * 2 + 1)
    own_copy = pltpu.make_async_copy(noisy, own, own_sem)
    own_copy.start()

    barrier = pltpu.get_barrier_semaphore()

    def signal(target):
        pl.semaphore_signal(barrier, inc=1, device_id=target, device_id_type=pl.DeviceIdType.LOGICAL)

    heard = []
    for dr, dc in SIDES:
        pl.when(exists(dr, dc))(lambda dr=dr, dc=dc: signal(ident(row + dr, col + dc)))
        heard.append(exists(dr, dc))

    def row_in(r):
        return (r >= 0) & (r < N_ROW)

    for k in (-1, 0, 1):
        for c in (2 * Y - 1, 2 * Y):
            pl.when(hub & row_in(hub_row + k))(lambda k=k, c=c: signal(ident(hub_row + k, c)))
        heard.append((before | after) & row_in(row + k))

    @pl.when(is_root)
    def _():
        for i in range(ROOTS):
            xx, yy = i // Y, i % Y

            @pl.when((x != xx) | (y != yy))
            def _():
                signal(ident(xx, yy * 2 + 1))

        signal(ident(row, col - 1))

        @pl.loop(1, Z)
        def _(zz):
            r, c = lax.rem(zz, Z_LO) * X + x, ((zz // Z_LO) * Y + y) * 2
            signal(ident(r, c))
            signal(ident(r, c + 1))


    gone = (
        (row == 0, top), (row == N_ROW - 1, bot), ((col == 0) | after, lef), ((col == N_COL - 1) | before, rig),
        (hub & (hub_row == 0), seam_up), (hub & (hub_row == N_ROW - 1), seam_down),
    )
    for cond, buf in gone:

        @pl.when(cond)
        def _():
            buf[...] = jnp.zeros_like(buf)

    for i, (dr, dc) in enumerate([(-1, -1), (-1, 1), (1, -1), (1, 1)]):

        @pl.when(jnp.logical_not(exists(dr, dc)))
        def _():
            corners[i] = jnp.zeros((8, 128), f32)

    for ref in (xs, pr):
        for t in range(NT + 2):
            ref[t, 0:BASE, :] = jnp.zeros((BASE, 128), f32)
            ref[t, BASE + FR : BUF, :] = jnp.zeros((BUF - BASE - FR, 128), f32)

    own_copy.wait()
    count = jnp.where(is_root, ROOTS - 1, 1)
    for hear in heard:
        count = count + jnp.where(hear, 1, 0)
    pl.semaphore_wait(barrier, count)

    place = {
        (-1, 0): top, (1, 0): bot, (0, -1): lef, (0, 1): rig, (-1, -1): corners.at[0], (-1, 1): corners.at[1],
        (1, -1): corners.at[2], (1, 1): corners.at[3],
    }

    def source(dr, dc):
        rs = slice(0, TR) if dr == 0 else slice(0, 8) if dr < 0 else slice(TR - 8, TR)
        cs = slice(0, TC) if dc == 0 else slice(0, 128) if dc < 0 else slice(TC - 128, TC)
        return own.at[rs, cs]

    def halo(dr, dc):
        i = SIDES.index((dr, dc))
        return pltpu.make_async_remote_copy(
            source(dr, dc), place[(-dr, -dc)], send_sem.at[i], recv_sem.at[SIDES.index((-dr, -dc))],
            device_id=ident(row + dr, col + dc), device_id_type=pl.DeviceIdType.LOGICAL,
        )

    def arrived(dr, dc):
        i = SIDES.index((dr, dc))
        return pltpu.make_async_remote_copy(
            source(-dr, -dc), place[(dr, dc)], send_sem.at[i], recv_sem.at[i],
            device_id=ident(row, col), device_id_type=pl.DeviceIdType.LOGICAL,
        )

    for dr, dc in [(1, 0), (-1, 0), (0, 1), (0, -1), (1, 1), (1, -1), (-1, 1), (-1, -1)]:
        pl.when(exists(dr, dc))(lambda dr=dr, dc=dc: halo(dr, dc).start())

    def to_hub(side, k):
        ref = (seam_down, seam_mid, seam_up)[k + 1]
        rs = (slice(0, 8), slice(0, TR), slice(TR - 8, TR))[k + 1]
        cs = (slice(TC - 128, TC), slice(0, 128))[side]
        i = side * 3 + k + 1
        return pltpu.make_async_remote_copy(
            own.at[rs, cs], ref.at[side], seam_send.at[k + 1], seam_recv.at[i],
            device_id=hub_of(row + k), device_id_type=pl.DeviceIdType.LOGICAL,
        )

    for side, here in enumerate((before, after)):
        for k in (0, -1, 1):
            pl.when(here & row_in(row + k))(lambda side=side, k=k: to_hub(side, k).start())

    def row_mask_of(r):
        grow = r * TR - TOP + sub
        return jnp.where((grow >= 0) & (grow < N_ROW * TR - 1), DSTEP, 0.0).astype(f32)

    rows_in = (sub >= TOP) & (sub < TOP + TR)

    def frame(ref, t, shift=0):
        return ref[t, BASE + shift : BASE + shift + FR, :]

    def left_of(v):
        return pltpu.roll(v, 1, 1)

    def right_of(v):
        return pltpu.roll(v, 127, 1)

    def sums(cell):
        acc = cell[0:8]
        for i in range(1, FR // 8):
            acc = acc + cell[8 * i : 8 * i + 8]
        return acc

    def sweeps(tiles, row_mask, col_mask, keep):
        acc_a, acc_b = [], []
        for k in range(ITERS):
            a_sum = b_sum = None
            prev_pc = None
            pend = None
            rolled_n = None
            for t in tiles + [None]:
                if t is not None:
                    n = frame(nf, t)
                    if k == 0:
                        ncol = right_of(n) if rolled_n is None else rolled_n
                        if t != tiles[-1]:
                            rolled_n = right_of(frame(nf, t + 1))
                            nright = jnp.where(lane == 127, rolled_n, ncol)
                        else:
                            nright = ncol
                        qr = (frame(nf, t, 1) - n) * row_mask
                        qc = (nright - n) * col_mask
                        gr[t] = qr
                        gc[t] = qc
                    else:
                        qr = frame(pr, t) + er[t]
                        qc = pc[t] + ec[t]
                    shrink = lax.rsqrt(jnp.maximum(qr * qr + qc * qc, 1.0))
                    p_r = qr * shrink
                    p_c = qc * shrink
                    pr[t, BASE : BASE + FR, :] = p_r
                    if k < ITERS - 1:
                        pc[t] = p_c
                    rolled = left_of(p_c)
                    pleft = rolled if prev_pc is None else jnp.where(lane == 0, prev_pc, rolled)
                    prev_pc = rolled
                    d = (p_r - frame(pr, t, -1)) + (p_c - pleft)
                    if k == 0:
                        new = n + KB * d
                        nc[t] = n * KC
                    else:
                        new = KA * frame(xs, t) + (KB * d + nc[t])
                    xs[t, BASE : BASE + FR, :] = new
                    rolled_x = right_of(new)
                if pend is not None:
                    s, sx, sd, sn, srolled = pend
                    xright = srolled if t is None else jnp.where(lane == 127, rolled_x, srolled)
                    g_r = (frame(xs, s, 1) - sx) * row_mask
                    g_c = (xright - sx) * col_mask
                    if k < ITERS - 1:
                        er[s] = g_r + (g_r - gr[s])
                        ec[s] = g_c + (g_c - gc[s])
                        gr[s] = g_r
                        gc[s] = g_c
                    m = g_r * g_r + g_c * g_c
                    size = m * lax.rsqrt(jnp.maximum(m, TINY))
                    diff = sx - sn
                    rest = (diff * diff) * (0.5 * FIDELITY) + sd * (sn + sd * (0.5 / FIDELITY))
                    mask = keep(s)
                    size = sums(jnp.where(mask, size, 0.0))
                    rest = sums(jnp.where(mask, rest, 0.0))
                    a_sum = size if a_sum is None else a_sum + size
                    b_sum = rest if b_sum is None else b_sum + rest
                if t is not None:
                    pend = (t, new, d, n, rolled_x)
            acc_a.append(a_sum)
            acc_b.append(b_sum)
        return acc_a, acc_b

    def wait_side(dr, dc):
        pl.when(exists(dr, dc))(lambda: arrived(dr, dc).wait_recv())

    wait_side(-1, 0)
    wait_side(1, 0)
    for t in range(NT):
        cs = slice(128 * t, 128 * t + 128)
        nf[t, BASE + TOP - 8 : BASE + TOP, :] = top[:, cs]
        nf[t, BASE + TOP : BASE + TOP + TR, :] = own[:, cs]
        nf[t, BASE + TOP + TR : BASE + TOP + TR + 8, :] = bot[:, cs]

    def keep_main(t):
        if t == 0:
            return rows_in & (lane >= EDGE)
        if t == NT - 1:
            return rows_in & (lane < 128 - EDGE)
        return rows_in

    acc_a, acc_b = sweeps(list(range(NT)), row_mask_of(row), DSTEP, keep_main)

    for dr in (-1, 0, 1):
        wait_side(dr, -1)
        wait_side(dr, 1)

    def pack(last, right, left, first):
        q = lax.broadcasted_iota(jnp.int32, last.shape, 1)
        v = jnp.where(q < 32, pltpu.roll(last, 32, 1), pltpu.roll(right, 32, 1))
        if left is None:
            return v
        w = jnp.where(q < 96, pltpu.roll(left, 96, 1), pltpu.roll(first, 96, 1))
        return jnp.where(q < 64, v, w)

    def fill(t, parts):
        nf[t, BASE + TOP - 8 : BASE + TOP, :] = parts[0]
        nf[t, BASE + TOP : BASE + TOP + TR, :] = parts[1]
        nf[t, BASE + TOP + TR : BASE + TOP + TR + 8, :] = parts[2]

    lo, hi = slice(0, 128), slice(TC - 128, TC)
    fill(STRIP, [
        pack(top[:, hi], corners[1], corners[0], top[:, lo]),
        pack(own[:, hi], rig[...], lef[...], own[:, lo]),
        pack(bot[:, hi], corners[3], corners[2], bot[:, lo]),
    ])
    outside = ((col == 0) & (lane >= 64) & (lane < 96)) | ((col == N_COL - 1) & (lane >= 31) & (lane < 64))
    strip_mask = jnp.where(outside, 0.0, DSTEP).astype(f32)
    owned = jnp.logical_not(before) & (lane >= 32 - EDGE) & (lane < 32)
    owned = owned | (jnp.logical_not(after) & (lane >= 96) & (lane < 96 + EDGE))
    owned = owned & rows_in
    strip_a, strip_b = sweeps([STRIP], row_mask_of(row), strip_mask, lambda t: owned)

    lane8 = lax.broadcasted_iota(jnp.int32, (8, 128), 1)
    sub8 = lax.broadcasted_iota(jnp.int32, (8, 128), 0)

    def line_of(a, b):
        table = jnp.zeros((8, 128), f32)
        for k in range(ITERS):
            total = a[k] * (1.0 / DSTEP) + b[k]
            table = jnp.where(sub8 == k, jnp.sum(total, axis=0, keepdims=True), table)
        line = jnp.sum(table, axis=1, keepdims=True)
        return jnp.sum(jnp.where(lane8 == sub8, line, 0.0), axis=0, keepdims=True)

    msg[...] = line_of([p + q for p, q in zip(acc_a, strip_a)], [p + q for p, q in zip(acc_b, strip_b)])

    slot = z * 2 + core
    part_copy = pltpu.make_async_remote_copy(
        msg, part.at[slot], part_send, part_recv, device_id=root_id, device_id_type=pl.DeviceIdType.LOGICAL
    )
    pl.when(jnp.logical_not(hub))(lambda: part_copy.start())

    lane32 = lax.broadcasted_iota(jnp.int32, (TR, 128), 1)
    for t in range(NT):
        v = xs[t, BASE + TOP : BASE + TOP + TR, :]
        if t in (0, NT - 1):
            s = xs[STRIP, BASE + TOP : BASE + TOP + TR, :]
            if t == 0:
                v = jnp.where(lane32 < EDGE, pltpu.roll(s, 32, 1), v)
            else:
                v = jnp.where(lane32 >= 128 - EDGE, pltpu.roll(s, 96, 1), v)
        out[:, 128 * t : 128 * t + 128] = v

    def back(c):
        return pltpu.make_async_remote_copy(
            seam_out, seam_in, back_send.at[c - (2 * Y - 1)], back_recv,
            device_id=ident(hub_row, c), device_id_type=pl.DeviceIdType.LOGICAL,
        )

    @pl.when(hub)
    def _():
        for side in (0, 1):
            for k in (-1, 0, 1):
                ref = (seam_up, seam_mid, seam_down)[k + 1]
                i = side * 3 - k + 1

                @pl.when(row_in(hub_row + k))
                def _():
                    pltpu.make_async_copy(ref.at[side], ref.at[side], seam_recv.at[i]).wait()

        fill(SEAM, [pack(ref[0], ref[1], None, None) for ref in (seam_up, seam_mid, seam_down)])
        inner = rows_in & (lane >= 32 - EDGE) & (lane < 32 + EDGE)
        seam_a, seam_b = sweeps([SEAM], row_mask_of(hub_row), DSTEP, lambda t: inner)
        seam_out[...] = xs[SEAM, BASE + TOP : BASE + TOP + TR, :]
        msg[...] = msg[...] + line_of(seam_a, seam_b)
        back(2 * Y - 1).start()
        back(2 * Y).start()
        pl.when(core != 1)(lambda: part_copy.start())

    for here, lanes, cols in (
        (before, lane32 >= 128 - EDGE, slice(TC - 128, TC)), (after, lane32 < EDGE, slice(0, 128))
    ):

        @pl.when(here)
        def _():
            pltpu.make_async_copy(seam_in, seam_in, back_recv).wait()
            out[:, cols] = jnp.where(lanes, pltpu.roll(seam_in[...], 96, 1), out[:, cols])

    def rows_of(ref, n, sem):
        return pltpu.make_async_copy(ref.at[0:n], ref.at[0:n], sem)

    @pl.when(is_root)
    def _():
        rows_of(part, 2 * Z - 1, part_recv).wait()
        part[1] = msg[...]
        total = part[0]
        for i in range(1, 2 * Z):
            total = total + part[i]
        me = x * Y + y
        plane[me] = total
        for i in range(ROOTS):
            xx, yy = i // Y, i % Y

            @pl.when((x != xx) | (y != yy))
            def _():
                pltpu.make_async_remote_copy(
                    plane.at[me], plane.at[me], plane_send, plane_recv,
                    device_id=ident(xx, yy * 2 + 1), device_id_type=pl.DeviceIdType.LOGICAL,
                ).start()

        rows_of(plane, ROOTS - 1, plane_recv).wait()
        total = plane[0]
        for i in range(1, ROOTS):
            total = total + plane[i]
        result[...] = total * (1.0 / CELLS)

        def tell(target):
            pltpu.make_async_remote_copy(
                result, result, result_send, result_recv, device_id=target, device_id_type=pl.DeviceIdType.LOGICAL
            ).start()

        tell(ident(row, col - 1))

        @pl.loop(1, Z)
        def _(zz):
            r, c = lax.rem(zz, Z_LO) * X + x, ((zz // Z_LO) * Y + y) * 2
            tell(ident(r, c))
            tell(ident(r, c + 1))

        gap[...] = result[...]
        rows_of(plane, ROOTS - 1, plane_send).wait()
        rows_of(part, 2 * Z - 1, result_send).wait()

    @pl.when(jnp.logical_not(is_root))
    def _():
        pltpu.make_async_copy(result, result, result_recv).wait()
        gap[...] = result[...]
        part_copy.wait_send()

    for dr, dc in SIDES:
        pl.when(exists(dr, dc))(lambda dr=dr, dc=dc: halo(dr, dc).wait_send())
    for side, here in enumerate((before, after)):
        for k in (-1, 0, 1):
            pl.when(here & row_in(row + k))(lambda side=side, k=k: to_hub(side, k).wait_send())

    @pl.when(hub)
    def _():
        back(2 * Y - 1).wait_send()
        back(2 * Y).wait_send()


def on_device(noisy):
    f32 = jnp.float32
    vmem = pl.BlockSpec(memory_space=pltpu.VMEM)
    frame = lambda rows: pltpu.VMEM((NT + 2, rows, 128), f32)
    dma = pltpu.SemaphoreType.DMA
    denoised, gap = pl.pallas_call(
        kernel,
        out_shape=(jax.ShapeDtypeStruct((TR, TC), f32), jax.ShapeDtypeStruct((1, 128), f32)),
        in_specs=[pl.BlockSpec(memory_space=pltpu.HBM)],
        out_specs=(vmem, vmem),
        scratch_shapes=[
            pltpu.VMEM((TR, TC), f32),
            pltpu.VMEM((8, TC), f32),
            pltpu.VMEM((8, TC), f32),
            pltpu.VMEM((TR, 128), f32),
            pltpu.VMEM((TR, 128), f32),
            pltpu.VMEM((4, 8, 128), f32),
            pltpu.VMEM((2, TR, 128), f32),
            pltpu.VMEM((2, 8, 128), f32),
            pltpu.VMEM((2, 8, 128), f32),
            pltpu.VMEM((TR, 128), f32),
            pltpu.VMEM((TR, 128), f32),
            frame(BUF), frame(FR), frame(BUF), frame(BUF), frame(FR), frame(FR), frame(FR), frame(FR), frame(FR),
            pltpu.VMEM((1, 128), f32),
            pltpu.VMEM((2 * Z, 1, 128), f32),
            pltpu.VMEM((ROOTS, 1, 128), f32),
            pltpu.VMEM((1, 128), f32),
            dma, dma((8,)), dma((8,)), dma, dma, dma, dma, dma, dma, dma((3,)), dma((6,)), dma((2,)), dma,
        ],
        compiler_params=pltpu.CompilerParams(
            collective_id=0, has_side_effects=True, vmem_limit_bytes=16 * 1024 * 1024
        ),
    )(pltpu.with_memory_space_constraint(noisy, pltpu.HBM))
    return denoised, gap[0, :ITERS]


def solution(mesh):
    return jax.shard_map(
        on_device,
        mesh=mesh,
        in_specs=(P("row", "col"),),
        out_specs=(P("row", "col"), P()),
        check_vma=False,
    )
```

```python
import jax
import jax.numpy as jnp
from jax import lax
from jax.experimental import pallas as pl
from jax.experimental.pallas import tpu as pltpu
from jax.sharding import PartitionSpec as P

ITERS = 4
Z_LO, X, Z_HI, Y = 8, 4, 2, 4
Z = Z_HI * Z_LO
N_ROW, N_COL = Z_LO * X, Z_HI * Y * 2
ROOTS = X * Y
TR, TC = 32, 2048
NT = TC // 128
FR = 40
BASE = 8
BUF = 56
TOP = 4
STRIP = NT
SEAM = NT + 1
EDGE = 8

FIDELITY = 8.0
PSTEP = 0.35
DSTEP = 0.35
KA = 1.0 / (1.0 + PSTEP * FIDELITY)
KB = PSTEP / (1.0 + PSTEP * FIDELITY)
KC = PSTEP * FIDELITY / (1.0 + PSTEP * FIDELITY)
CELLS = float(N_ROW * TR * N_COL * TC)
TINY = 1e-37

SIDES = [(dr, dc) for dr in (-1, 0, 1) for dc in (-1, 0, 1) if (dr, dc) != (0, 0)]


def kernel(
    noisy, out, gap, own, top, bot, lef, rig, corners, seam_mid, seam_up, seam_down, seam_out, seam_in, nf, nc, xs, pr, pc, er, ec, gr, gc,
    msg, part, result, own_sem, send_sem, recv_sem, part_send, part_recv,
    result_send, result_recv, seam_send, seam_recv, back_send, back_recv,
):
    f32 = jnp.float32
    row, col = lax.axis_index("row"), lax.axis_index("col")
    zl, x = row // X, row % X
    zh, y, core = col // (2 * Y), (col // 2) % Y, col % 2
    z = zh * Z_LO + zl
    lane = lax.broadcasted_iota(jnp.int32, (FR, 128), 1)
    sub = lax.broadcasted_iota(jnp.int32, (FR, 128), 0)
    is_root = (z == 0) & (core == 1)
    before, after = col == 2 * Y - 1, col == 2 * Y
    hub = z == 0
    hub_row = col * X + x

    def ident(r, c):
        return r * N_COL + c

    def hub_of(r):
        return ident(r % X, r // X)

    def exists(dr, dc):
        cond = jnp.logical_not(before if dc > 0 else after) if dc else None
        for t in ([row >= 1] if dr < 0 else [row < N_ROW - 1] if dr > 0 else []) + (
            [col >= 1] if dc < 0 else [col < N_COL - 1] if dc > 0 else []
        ):
            cond = t if cond is None else cond & t
        return cond

    own_copy = pltpu.make_async_copy(noisy, own, own_sem)
    own_copy.start()

    barrier = pltpu.get_barrier_semaphore()

    def signal(target):
        pl.semaphore_signal(barrier, inc=1, device_id=target, device_id_type=pl.DeviceIdType.LOGICAL)

    heard = []
    for dr, dc in SIDES:
        pl.when(exists(dr, dc))(lambda dr=dr, dc=dc: signal(ident(row + dr, col + dc)))
        heard.append(exists(dr, dc))

    def row_in(r):
        return (r >= 0) & (r < N_ROW)

    for k in (-1, 0, 1):
        for c in (2 * Y - 1, 2 * Y):
            pl.when(hub & row_in(hub_row + k))(lambda k=k, c=c: signal(ident(hub_row + k, c)))
        heard.append((before | after) & row_in(row + k))

    @pl.when(is_root)
    def _():
        @pl.loop(0, Z - 1)
        def _(i):
            step = (i + 1) // 2
            zz = jnp.where(i % 2 == 1, Z // 2 - step, Z // 2 + step)
            for xx in range(X):
                for yc in range(2 * Y):
                    signal(ident((zz % Z_LO) * X + xx, (zz // Z_LO) * 2 * Y + yc))

        for xx in range(X):
            for yc in range(2 * Y):
                pl.when((x != xx) | (y * 2 + 1 != yc))(lambda xx=xx, yc=yc: signal(ident(xx, yc)))

    gone = (
        (row == 0, top), (row == N_ROW - 1, bot), ((col == 0) | after, lef), ((col == N_COL - 1) | before, rig),
        (hub & (hub_row == 0), seam_up), (hub & (hub_row == N_ROW - 1), seam_down),
    )
    for cond, buf in gone:

        @pl.when(cond)
        def _():
            buf[...] = jnp.zeros_like(buf)

    for i, (dr, dc) in enumerate([(-1, -1), (-1, 1), (1, -1), (1, 1)]):

        @pl.when(jnp.logical_not(exists(dr, dc)))
        def _():
            corners[i] = jnp.zeros((8, 128), f32)

    for ref in (xs, pr):
        for t in range(NT + 2):
            ref[t, 0:BASE, :] = jnp.zeros((BASE, 128), f32)
            ref[t, BASE + FR : BUF, :] = jnp.zeros((BUF - BASE - FR, 128), f32)

    own_copy.wait()
    count = jnp.where(is_root, ROOTS - 1, ROOTS)
    for hear in heard:
        count = count + jnp.where(hear, 1, 0)
    pl.semaphore_wait(barrier, count)

    place0 = {
        (-1, 0): top, (1, 0): bot, (0, -1): lef, (0, 1): rig, (-1, -1): corners.at[0], (-1, 1): corners.at[1],
        (1, -1): corners.at[2], (1, 1): corners.at[3],
    }

    place = {k: (v if k[0] == 0 else v.at[4:8] if k[0] < 0 else v.at[0:5]) for k, v in place0.items()}

    def source(dr, dc):
        rs = slice(0, TR) if dr == 0 else slice(0, 5) if dr < 0 else slice(TR - 4, TR)
        cs = slice(0, TC) if dc == 0 else slice(0, 128) if dc < 0 else slice(TC - 128, TC)
        return own.at[rs, cs]

    def halo(dr, dc):
        i = SIDES.index((dr, dc))
        return pltpu.make_async_remote_copy(
            source(dr, dc), place[(-dr, -dc)], send_sem.at[i], recv_sem.at[SIDES.index((-dr, -dc))],
            device_id=ident(row + dr, col + dc), device_id_type=pl.DeviceIdType.LOGICAL,
        )

    def arrived(dr, dc):
        i = SIDES.index((dr, dc))
        return pltpu.make_async_remote_copy(
            source(-dr, -dc), place[(dr, dc)], send_sem.at[i], recv_sem.at[i],
            device_id=ident(row, col), device_id_type=pl.DeviceIdType.LOGICAL,
        )

    for dr, dc in [(1, 0), (-1, 0), (0, 1), (0, -1), (1, 1), (1, -1), (-1, 1), (-1, -1)]:
        pl.when(exists(dr, dc))(lambda dr=dr, dc=dc: halo(dr, dc).start())

    def to_hub(side, k):
        ref = (seam_down, seam_mid, seam_up)[k + 1]
        rs = (slice(0, 8), slice(0, TR), slice(TR - 8, TR))[k + 1]
        cs = (slice(TC - 128, TC), slice(0, 128))[side]
        i = side * 3 + k + 1
        return pltpu.make_async_remote_copy(
            own.at[rs, cs], ref.at[side], seam_send.at[k + 1], seam_recv.at[i],
            device_id=hub_of(row + k), device_id_type=pl.DeviceIdType.LOGICAL,
        )

    for side, here in enumerate((before, after)):
        for k in (0, -1, 1):
            pl.when(here & row_in(row + k))(lambda side=side, k=k: to_hub(side, k).start())

    def row_mask_of(r):
        grow = r * TR - TOP + sub
        return jnp.where((grow >= 0) & (grow < N_ROW * TR - 1), DSTEP, 0.0).astype(f32)

    rows_in = (sub >= TOP) & (sub < TOP + TR)

    def frame(ref, t, shift=0):
        return ref[t, BASE + shift : BASE + shift + FR, :]

    def left_of(v):
        return pltpu.roll(v, 1, 1)

    def right_of(v):
        return pltpu.roll(v, 127, 1)

    def sums(cell):
        acc = cell[0:8]
        for i in range(1, FR // 8):
            acc = acc + cell[8 * i : 8 * i + 8]
        return acc

    def sweeps(tiles, row_mask, col_mask, keep):
        acc_a, acc_b = [], []
        for k in range(ITERS):
            a_sum = b_sum = None
            prev_pc = None
            pend = None
            rolled_n = None
            for t in tiles + [None]:
                if t is not None:
                    n = frame(nf, t)
                    if k == 0:
                        ncol = right_of(n) if rolled_n is None else rolled_n
                        if t != tiles[-1]:
                            rolled_n = right_of(frame(nf, t + 1))
                            nright = jnp.where(lane == 127, rolled_n, ncol)
                        else:
                            nright = ncol
                        qr = (frame(nf, t, 1) - n) * row_mask
                        qc = (nright - n) * col_mask
                        gr[t] = qr
                        gc[t] = qc
                    else:
                        qr = frame(pr, t) + er[t]
                        qc = pc[t] + ec[t]
                    shrink = lax.rsqrt(jnp.maximum(qr * qr + qc * qc, 1.0))
                    p_r = qr * shrink
                    p_c = qc * shrink
                    pr[t, BASE : BASE + FR, :] = p_r
                    if k < ITERS - 1:
                        pc[t] = p_c
                    rolled = left_of(p_c)
                    pleft = rolled if prev_pc is None else jnp.where(lane == 0, prev_pc, rolled)
                    prev_pc = rolled
                    d = (p_r - frame(pr, t, -1)) + (p_c - pleft)
                    if k == 0:
                        new = n + KB * d
                        nc[t] = n * KC
                    else:
                        new = KA * frame(xs, t) + (KB * d + nc[t])
                    xs[t, BASE : BASE + FR, :] = new
                    rolled_x = right_of(new)
                if pend is not None:
                    s, sx, sd, sn, srolled = pend
                    xright = srolled if t is None else jnp.where(lane == 127, rolled_x, srolled)
                    g_r = (frame(xs, s, 1) - sx) * row_mask
                    g_c = (xright - sx) * col_mask
                    if k < ITERS - 1:
                        er[s] = g_r + (g_r - gr[s])
                        ec[s] = g_c + (g_c - gc[s])
                        gr[s] = g_r
                        gc[s] = g_c
                    m = g_r * g_r + g_c * g_c
                    size = m * lax.rsqrt(jnp.maximum(m, TINY))
                    diff = sx - sn
                    rest = (diff * diff) * (0.5 * FIDELITY) + sd * (sn + sd * (0.5 / FIDELITY))
                    mask = keep(s)
                    size = sums(jnp.where(mask, size, 0.0))
                    rest = sums(jnp.where(mask, rest, 0.0))
                    a_sum = size if a_sum is None else a_sum + size
                    b_sum = rest if b_sum is None else b_sum + rest
                if t is not None:
                    pend = (t, new, d, n, rolled_x)
            acc_a.append(a_sum)
            acc_b.append(b_sum)
        return acc_a, acc_b

    def wait_side(dr, dc):
        pl.when(exists(dr, dc))(lambda: arrived(dr, dc).wait_recv())

    wait_side(-1, 0)
    wait_side(1, 0)
    for t in range(NT):
        cs = slice(128 * t, 128 * t + 128)
        nf[t, BASE + TOP - 8 : BASE + TOP, :] = top[:, cs]
        nf[t, BASE + TOP : BASE + TOP + TR, :] = own[:, cs]
        nf[t, BASE + TOP + TR : BASE + TOP + TR + 8, :] = bot[:, cs]

    def keep_main(t):
        if t == 0:
            return rows_in & (lane >= EDGE)
        if t == NT - 1:
            return rows_in & (lane < 128 - EDGE)
        return rows_in

    acc_a, acc_b = sweeps(list(range(NT)), row_mask_of(row), DSTEP, keep_main)

    for dr in (-1, 0, 1):
        wait_side(dr, -1)
        wait_side(dr, 1)

    def pack(last, right, left, first):
        q = lax.broadcasted_iota(jnp.int32, last.shape, 1)
        v = jnp.where(q < 32, pltpu.roll(last, 32, 1), pltpu.roll(right, 32, 1))
        if left is None:
            return v
        w = jnp.where(q < 96, pltpu.roll(left, 96, 1), pltpu.roll(first, 96, 1))
        return jnp.where(q < 64, v, w)

    def fill(t, parts):
        nf[t, BASE + TOP - 8 : BASE + TOP, :] = parts[0]
        nf[t, BASE + TOP : BASE + TOP + TR, :] = parts[1]
        nf[t, BASE + TOP + TR : BASE + TOP + TR + 8, :] = parts[2]

    lo, hi = slice(0, 128), slice(TC - 128, TC)
    fill(STRIP, [
        pack(top[:, hi], corners[1], corners[0], top[:, lo]),
        pack(own[:, hi], rig[...], lef[...], own[:, lo]),
        pack(bot[:, hi], corners[3], corners[2], bot[:, lo]),
    ])
    outside = ((col == 0) & (lane >= 64) & (lane < 96)) | ((col == N_COL - 1) & (lane >= 31) & (lane < 64))
    strip_mask = jnp.where(outside, 0.0, DSTEP).astype(f32)
    owned = jnp.logical_not(before) & (lane >= 32 - EDGE) & (lane < 32)
    owned = owned | (jnp.logical_not(after) & (lane >= 96) & (lane < 96 + EDGE))
    owned = owned & rows_in
    strip_a, strip_b = sweeps([STRIP], row_mask_of(row), strip_mask, lambda t: owned)

    lane8 = lax.broadcasted_iota(jnp.int32, (8, 128), 1)
    sub8 = lax.broadcasted_iota(jnp.int32, (8, 128), 0)

    def line_of(a, b):
        table = jnp.zeros((8, 128), f32)
        for k in range(ITERS):
            total = a[k] * (1.0 / DSTEP) + b[k]
            table = jnp.where(sub8 == k, jnp.sum(total, axis=0, keepdims=True), table)
        line = jnp.sum(table, axis=1, keepdims=True)
        return jnp.sum(jnp.where(lane8 == sub8, line, 0.0), axis=0, keepdims=True)

    msg[...] = line_of([p + q for p, q in zip(acc_a, strip_a)], [p + q for p, q in zip(acc_b, strip_b)])

    slot = ident(row, col)

    def send_sums():
        for i in range(ROOTS):
            xx, yc = i // Y, i % Y * 2 + 1

            @pl.when((row != xx) | (col != yc))
            def _():
                pltpu.make_async_remote_copy(
                    msg, part.at[slot], part_send, part_recv,
                    device_id=ident(xx, yc), device_id_type=pl.DeviceIdType.LOGICAL,
                ).start()

    pl.when(jnp.logical_not(hub))(send_sums)

    lane32 = lax.broadcasted_iota(jnp.int32, (TR, 128), 1)
    for t in range(NT):
        v = xs[t, BASE + TOP : BASE + TOP + TR, :]
        if t in (0, NT - 1):
            s = xs[STRIP, BASE + TOP : BASE + TOP + TR, :]
            if t == 0:
                v = jnp.where(lane32 < EDGE, pltpu.roll(s, 32, 1), v)
            else:
                v = jnp.where(lane32 >= 128 - EDGE, pltpu.roll(s, 96, 1), v)
        out[:, 128 * t : 128 * t + 128] = v

    def back(c):
        return pltpu.make_async_remote_copy(
            seam_out, seam_in, back_send.at[c - (2 * Y - 1)], back_recv,
            device_id=ident(hub_row, c), device_id_type=pl.DeviceIdType.LOGICAL,
        )

    @pl.when(hub)
    def _():
        for side in (0, 1):
            for k in (-1, 0, 1):
                ref = (seam_up, seam_mid, seam_down)[k + 1]
                i = side * 3 - k + 1

                @pl.when(row_in(hub_row + k))
                def _():
                    pltpu.make_async_copy(ref.at[side], ref.at[side], seam_recv.at[i]).wait()

        fill(SEAM, [pack(ref[0], ref[1], None, None) for ref in (seam_up, seam_mid, seam_down)])
        inner = rows_in & (lane >= 32 - EDGE) & (lane < 32 + EDGE)
        seam_a, seam_b = sweeps([SEAM], row_mask_of(hub_row), DSTEP, lambda t: inner)
        seam_out[...] = xs[SEAM, BASE + TOP : BASE + TOP + TR, :]
        msg[...] = msg[...] + line_of(seam_a, seam_b)
        back(2 * Y - 1).start()
        back(2 * Y).start()
        send_sums()

    for here, lanes, cols in (
        (before, lane32 >= 128 - EDGE, slice(TC - 128, TC)), (after, lane32 < EDGE, slice(0, 128))
    ):

        @pl.when(here)
        def _():
            pltpu.make_async_copy(seam_in, seam_in, back_recv).wait()
            out[:, cols] = jnp.where(lanes, pltpu.roll(seam_in[...], 96, 1), out[:, cols])

    def rows_of(ref, n, sem):
        return pltpu.make_async_copy(ref.at[0:n], ref.at[0:n], sem)

    @pl.when(is_root)
    def _():
        part[slot] = msg[...]
        rows_of(part, N_ROW * N_COL - 1, part_recv).wait()
        total = jnp.sum(part[...], axis=0)
        result[...] = total * (1.0 / CELLS)

        def tell(target):
            pltpu.make_async_remote_copy(
                result, result, result_send, result_recv, device_id=target, device_id_type=pl.DeviceIdType.LOGICAL
            ).start()

        tell(ident(row, col - 1))

        @pl.loop(1, Z)
        def _(zz):
            r, c = lax.rem(zz, Z_LO) * X + x, ((zz // Z_LO) * Y + y) * 2
            tell(ident(r, c))
            tell(ident(r, c + 1))

        gap[...] = result[...]
        rows_of(part, 2 * Z - 1, result_send).wait()
        rows_of(part, ROOTS - 1, part_send).wait()

    @pl.when(jnp.logical_not(is_root))
    def _():
        pltpu.make_async_copy(result, result, result_recv).wait()
        gap[...] = result[...]
        rows_of(part, ROOTS, part_send).wait()

    for dr, dc in SIDES:
        pl.when(exists(dr, dc))(lambda dr=dr, dc=dc: halo(dr, dc).wait_send())
    for side, here in enumerate((before, after)):
        for k in (-1, 0, 1):
            pl.when(here & row_in(row + k))(lambda side=side, k=k: to_hub(side, k).wait_send())

    @pl.when(hub)
    def _():
        back(2 * Y - 1).wait_send()
        back(2 * Y).wait_send()


def finish(denoised, line, out, gap):
    out[...] = denoised[...]
    gap[...] = line[0, :ITERS]


def on_device(noisy):
    f32 = jnp.float32
    vmem = pl.BlockSpec(memory_space=pltpu.VMEM)
    frame = lambda rows: pltpu.VMEM((NT + 2, rows, 128), f32)
    dma = pltpu.SemaphoreType.DMA
    denoised, gap = pl.pallas_call(
        kernel,
        out_shape=(jax.ShapeDtypeStruct((TR, TC), f32), jax.ShapeDtypeStruct((1, 128), f32)),
        in_specs=[pl.BlockSpec(memory_space=pltpu.HBM)],
        out_specs=(vmem, vmem),
        scratch_shapes=[
            pltpu.VMEM((TR, TC), f32),
            pltpu.VMEM((8, TC), f32),
            pltpu.VMEM((8, TC), f32),
            pltpu.VMEM((TR, 128), f32),
            pltpu.VMEM((TR, 128), f32),
            pltpu.VMEM((4, 8, 128), f32),
            pltpu.VMEM((2, TR, 128), f32),
            pltpu.VMEM((2, 8, 128), f32),
            pltpu.VMEM((2, 8, 128), f32),
            pltpu.VMEM((TR, 128), f32),
            pltpu.VMEM((TR, 128), f32),
            frame(BUF), frame(FR), frame(BUF), frame(BUF), frame(FR), frame(FR), frame(FR), frame(FR), frame(FR),
            pltpu.VMEM((1, 128), f32),
            pltpu.VMEM((N_ROW * N_COL, 1, 128), f32),
            pltpu.VMEM((1, 128), f32),
            dma, dma((8,)), dma((8,)), dma, dma, dma, dma, dma((3,)), dma((6,)), dma((2,)), dma,
        ],
        compiler_params=pltpu.CompilerParams(
            collective_id=0, has_side_effects=True, vmem_limit_bytes=16 * 1024 * 1024
        ),
    )(pltpu.with_memory_space_constraint(noisy, pltpu.HBM))
    return pl.pallas_call(
        finish,
        out_shape=(jax.ShapeDtypeStruct((TR, TC), f32), jax.ShapeDtypeStruct((ITERS,), f32)),
        in_specs=[vmem, vmem],
        out_specs=(vmem, vmem),
        compiler_params=pltpu.CompilerParams(vmem_limit_bytes=4 * 1024 * 1024),
    )(denoised, gap)


def solution(mesh):
    return jax.shard_map(
        on_device,
        mesh=mesh,
        in_specs=(P("row", "col"),),
        out_specs=(P("row", "col"), P()),
        check_vma=False,
    )
```

```python
import jax
import jax.numpy as jnp
from jax import lax
from jax.experimental import pallas as pl
from jax.experimental.pallas import tpu as pltpu
from jax.sharding import PartitionSpec as P

ITERS = 4
Z_LO, X, Z_HI, Y = 8, 4, 2, 4
Z = Z_HI * Z_LO
N_ROW, N_COL = Z_LO * X, Z_HI * Y * 2
ROOTS = X * Y
TR, TC = 32, 2048
NT = TC // 128
FR = 40
BASE = 8
BUF = 56
TOP = 4
STRIP = NT
SEAM = NT + 1
EDGE = 8

FIDELITY = 8.0
PSTEP = 0.35
DSTEP = 0.35
KA = 1.0 / (1.0 + PSTEP * FIDELITY)
KB = PSTEP / (1.0 + PSTEP * FIDELITY)
KC = PSTEP * FIDELITY / (1.0 + PSTEP * FIDELITY)
CELLS = float(N_ROW * TR * N_COL * TC)
TINY = 1e-37

SIDES = [(dr, dc) for dr in (-1, 0, 1) for dc in (-1, 0, 1) if (dr, dc) != (0, 0)]


def kernel(
    noisy, out, gap, own, top, bot, lef, rig, corners, seam_mid, seam_up, seam_down, seam_out, seam_in, xs, pr, pc, er, ec, gr, gc,
    msg, part, result, own_sem, send_sem, recv_sem, part_send, part_recv,
    result_send, result_recv, seam_send, seam_recv, back_send, back_recv,
):
    f32 = jnp.float32
    row, col = lax.axis_index("row"), lax.axis_index("col")
    zl, x = row // X, row % X
    zh, y, core = col // (2 * Y), (col // 2) % Y, col % 2
    z = zh * Z_LO + zl

    def lane_of(wins):
        return lax.broadcasted_iota(jnp.int32, (sum(n for _, n in wins), 128), 1)

    def row_of(wins):
        return jnp.concatenate([a + lax.broadcasted_iota(jnp.int32, (n, 128), 0) for a, n in wins], axis=0)

    is_root = (z == 0) & (core == 1)
    before, after = col == 2 * Y - 1, col == 2 * Y
    hub = z == 0
    hub_row = col * X + x

    def ident(r, c):
        return r * N_COL + c

    def hub_of(r):
        return ident(r % X, r // X)

    def exists(dr, dc):
        cond = jnp.logical_not(before if dc > 0 else after) if dc else None
        for t in ([row >= 1] if dr < 0 else [row < N_ROW - 1] if dr > 0 else []) + (
            [col >= 1] if dc < 0 else [col < N_COL - 1] if dc > 0 else []
        ):
            cond = t if cond is None else cond & t
        return cond

    own_copy = pltpu.make_async_copy(noisy, own, own_sem)
    own_copy.start()

    barrier = pltpu.get_barrier_semaphore()

    def signal(target):
        pl.semaphore_signal(barrier, inc=1, device_id=target, device_id_type=pl.DeviceIdType.LOGICAL)

    heard = []
    for dr, dc in SIDES:
        pl.when(exists(dr, dc))(lambda dr=dr, dc=dc: signal(ident(row + dr, col + dc)))
        heard.append(exists(dr, dc))

    def row_in(r):
        return (r >= 0) & (r < N_ROW)

    for k in (-1, 0, 1):
        for c in (2 * Y - 1, 2 * Y):
            pl.when(hub & row_in(hub_row + k))(lambda k=k, c=c: signal(ident(hub_row + k, c)))
        heard.append((before | after) & row_in(row + k))

    @pl.when(is_root)
    def _():
        @pl.loop(0, Z - 1)
        def _(i):
            step = (i + 1) // 2
            zz = jnp.where(i % 2 == 1, Z // 2 - step, Z // 2 + step)
            for xx in range(X):
                for yc in range(2 * Y):
                    signal(ident((zz % Z_LO) * X + xx, (zz // Z_LO) * 2 * Y + yc))

        for xx in range(X):
            for yc in range(2 * Y):
                pl.when((x != xx) | (y * 2 + 1 != yc))(lambda xx=xx, yc=yc: signal(ident(xx, yc)))

    gone = (
        (row == 0, top), (row == N_ROW - 1, bot), ((col == 0) | after, lef), ((col == N_COL - 1) | before, rig),
        (hub & (hub_row == 0), seam_up), (hub & (hub_row == N_ROW - 1), seam_down),
    )
    for cond, buf in gone:

        @pl.when(cond)
        def _():
            buf[...] = jnp.zeros_like(buf)

    for i, (dr, dc) in enumerate([(-1, -1), (-1, 1), (1, -1), (1, 1)]):

        @pl.when(jnp.logical_not(exists(dr, dc)))
        def _():
            corners[i] = jnp.zeros((8, 128), f32)

    for k in range(ITERS):
        for t in range(NT + 2):
            pr[k, t, 0:BASE, :] = jnp.zeros((BASE, 128), f32)

    own_copy.wait()
    count = jnp.where(is_root, ROOTS - 1, ROOTS)
    for hear in heard:
        count = count + jnp.where(hear, 1, 0)
    pl.semaphore_wait(barrier, count)

    place0 = {
        (-1, 0): top, (1, 0): bot, (0, -1): lef, (0, 1): rig, (-1, -1): corners.at[0], (-1, 1): corners.at[1],
        (1, -1): corners.at[2], (1, 1): corners.at[3],
    }

    place = {k: (v if k[0] == 0 else v.at[4:8] if k[0] < 0 else v.at[0:5]) for k, v in place0.items()}

    def source(dr, dc):
        rs = slice(0, TR) if dr == 0 else slice(0, 5) if dr < 0 else slice(TR - 4, TR)
        cs = slice(0, TC) if dc == 0 else slice(0, 128) if dc < 0 else slice(TC - 128, TC)
        return own.at[rs, cs]

    def halo(dr, dc):
        i = SIDES.index((dr, dc))
        return pltpu.make_async_remote_copy(
            source(dr, dc), place[(-dr, -dc)], send_sem.at[i], recv_sem.at[SIDES.index((-dr, -dc))],
            device_id=ident(row + dr, col + dc), device_id_type=pl.DeviceIdType.LOGICAL,
        )

    def arrived(dr, dc):
        i = SIDES.index((dr, dc))
        return pltpu.make_async_remote_copy(
            source(-dr, -dc), place[(dr, dc)], send_sem.at[i], recv_sem.at[i],
            device_id=ident(row, col), device_id_type=pl.DeviceIdType.LOGICAL,
        )

    for dr, dc in [(1, 0), (-1, 0), (0, 1), (0, -1), (1, 1), (1, -1), (-1, 1), (-1, -1)]:
        pl.when(exists(dr, dc))(lambda dr=dr, dc=dc: halo(dr, dc).start())

    def to_hub(side, k):
        ref = (seam_down, seam_mid, seam_up)[k + 1]
        rs = (slice(0, 8), slice(0, TR), slice(TR - 8, TR))[k + 1]
        cs = (slice(TC - 128, TC), slice(0, 128))[side]
        i = side * 3 + k + 1
        return pltpu.make_async_remote_copy(
            own.at[rs, cs], ref.at[side], seam_send.at[k + 1], seam_recv.at[i],
            device_id=hub_of(row + k), device_id_type=pl.DeviceIdType.LOGICAL,
        )

    for side, here in enumerate((before, after)):
        for k in (0, -1, 1):
            pl.when(here & row_in(row + k))(lambda side=side, k=k: to_hub(side, k).start())

    def row_mask_of(r, wins):
        grow = r * TR - TOP + row_of(wins)
        return jnp.where((grow >= 0) & (grow < N_ROW * TR - 1), DSTEP, 0.0).astype(f32)

    def load(ref, k, t, wins, shift=0):
        return jnp.concatenate([ref[k, t, BASE + a + shift : BASE + a + shift + n, :] for a, n in wins], axis=0)

    def store(ref, k, t, wins, v):
        at = 0
        for a, n in wins:
            ref[k, t, BASE + a : BASE + a + n, :] = v[at : at + n]
            at += n

    def left_of(v):
        return pltpu.roll(v, 1, 1)

    def right_of(v):
        return pltpu.roll(v, 127, 1)

    def sums(cell):
        acc = cell[0:8]
        for i in range(1, cell.shape[0] // 8):
            acc = acc + cell[8 * i : 8 * i + 8]
        return acc

    def sweep(k, tiles, wins, row_mask, col_mask, keep):
        a_sum = b_sum = prev_pc = pend = rolled_n = None
        lane = lane_of(wins)
        for t in tiles + [None]:
            if t is not None:
                n = load(xs, 0, t, wins)
                if k == 0:
                    ncol = right_of(n) if rolled_n is None else rolled_n
                    nright = ncol
                    if t != tiles[-1]:
                        rolled_n = right_of(load(xs, 0, t + 1, wins))
                        nright = jnp.where(lane == 127, rolled_n, ncol)
                    qr = (load(xs, 0, t, wins, 1) - n) * row_mask
                    qc = (nright - n) * col_mask
                    store(gr, 0, t, wins, qr)
                    store(gc, 0, t, wins, qc)
                else:
                    qr = load(pr, k - 1, t, wins) + load(er, k - 1, t, wins)
                    qc = load(pc, k - 1, t, wins) + load(ec, k - 1, t, wins)
                shrink = lax.rsqrt(jnp.maximum(qr * qr + qc * qc, 1.0))
                p_r = qr * shrink
                p_c = qc * shrink
                store(pr, k, t, wins, p_r)
                if k < ITERS - 1:
                    store(pc, k, t, wins, p_c)
                rolled = left_of(p_c)
                pleft = rolled if prev_pc is None else jnp.where(lane == 0, prev_pc, rolled)
                prev_pc = rolled
                d = (p_r - load(pr, k, t, wins, -1)) + (p_c - pleft)
                if k == 0:
                    new = n + KB * d
                else:
                    new = KA * load(xs, k, t, wins) + (KB * d + KC * n)
                store(xs, k + 1, t, wins, new)
                rolled_x = right_of(new)
            if pend is not None:
                s, sx, sd, sn, srolled = pend
                xright = srolled if t is None else jnp.where(lane == 127, rolled_x, srolled)
                g_r = (load(xs, k + 1, s, wins, 1) - sx) * row_mask
                g_c = (xright - sx) * col_mask
                if k < ITERS - 1:
                    store(er, k, s, wins, g_r + (g_r - load(gr, k, s, wins)))
                    store(ec, k, s, wins, g_c + (g_c - load(gc, k, s, wins)))
                if k < ITERS - 2:
                    store(gr, k + 1, s, wins, g_r)
                    store(gc, k + 1, s, wins, g_c)
                m = g_r * g_r + g_c * g_c
                size = m * lax.rsqrt(jnp.maximum(m, TINY))
                diff = sx - sn
                rest = (diff * diff) * (0.5 * FIDELITY) + sd * (sn + sd * (0.5 / FIDELITY))
                mask = keep(s, lane)
                size = sums(jnp.where(mask, size, 0.0))
                rest = sums(jnp.where(mask, rest, 0.0))
                a_sum = size if a_sum is None else a_sum + size
                b_sum = rest if b_sum is None else b_sum + rest
            if t is not None:
                pend = (t, new, d, n, rolled_x)
        return a_sum, b_sum

    def wait_side(dr, dc):
        pl.when(exists(dr, dc))(lambda: arrived(dr, dc).wait_recv())

    def columns(t, lane):
        if t == 0:
            return lane >= EDGE
        if t == NT - 1:
            return lane < 128 - EDGE
        return None

    def keep_rows(wins, first, last):
        a = row_of(wins)
        inside = (a >= TOP + first) & (a <= TOP + last)

        def keep(t, lane):
            here = columns(t, lane)
            return inside if here is None else inside & here

        return keep

    MAIN = list(range(NT))
    FULL = [(0, FR)]
    INNER = [(TOP, TR)]
    for t in MAIN:
        xs[0, t, BASE + TOP : BASE + TOP + TR, :] = own[:, 128 * t : 128 * t + 128]
    inner_mask = row_mask_of(row, INNER)
    acc = []
    for k in range(ITERS):
        acc.append(sweep(k, MAIN, INNER, inner_mask, DSTEP, keep_rows(INNER, k + 1, TR - 3 - k)))

    wait_side(-1, 0)
    wait_side(1, 0)
    for dr in (-1, 0, 1):
        wait_side(dr, -1)
        wait_side(dr, 1)
    for t in MAIN:
        cs = slice(128 * t, 128 * t + 128)
        xs[0, t, BASE + TOP - 8 : BASE + TOP, :] = top[:, cs]
        xs[0, t, BASE + TOP + TR : BASE + TOP + TR + 8, :] = bot[:, cs]

    def pack(last, right, left, first):
        q = lax.broadcasted_iota(jnp.int32, last.shape, 1)
        v = jnp.where(q < 32, pltpu.roll(last, 32, 1), pltpu.roll(right, 32, 1))
        if left is None:
            return v
        w = jnp.where(q < 96, pltpu.roll(left, 96, 1), pltpu.roll(first, 96, 1))
        return jnp.where(q < 64, v, w)

    def fill(t, parts):
        xs[0, t, BASE + TOP - 8 : BASE + TOP, :] = parts[0]
        xs[0, t, BASE + TOP : BASE + TOP + TR, :] = parts[1]
        xs[0, t, BASE + TOP + TR : BASE + TOP + TR + 8, :] = parts[2]

    lo, hi = slice(0, 128), slice(TC - 128, TC)
    fill(STRIP, [
        pack(top[:, hi], corners[1], corners[0], top[:, lo]),
        pack(own[:, hi], rig[...], lef[...], own[:, lo]),
        pack(bot[:, hi], corners[3], corners[2], bot[:, lo]),
    ])
    lane = lane_of(FULL)
    outside = ((col == 0) & (lane >= 64) & (lane < 96)) | ((col == N_COL - 1) & (lane >= 31) & (lane < 64))
    strip_mask = jnp.where(outside, 0.0, DSTEP).astype(f32)
    rows_in = (row_of(FULL) >= TOP) & (row_of(FULL) < TOP + TR)
    owned = jnp.logical_not(before) & (lane >= 32 - EDGE) & (lane < 32)
    owned = owned | (jnp.logical_not(after) & (lane >= 96) & (lane < 96 + EDGE))
    owned = owned & rows_in
    full_mask = row_mask_of(row, FULL)
    for k in range(ITERS):
        wins = [(k, 8), (32 - k, 8)]
        rows = row_of(wins)
        edge = ((rows >= TOP) & (rows <= TOP + k)) | ((rows >= TOP + TR - 2 - k) & (rows < TOP + TR))

        def keep(t, lane, edge=edge):
            here = columns(t, lane)
            return edge if here is None else edge & here

        outer = sweep(k, MAIN, wins, row_mask_of(row, wins), DSTEP, keep)
        strip = sweep(k, [STRIP], FULL, full_mask, strip_mask, lambda t, lane: owned)
        acc[k] = tuple(p + q + r for p, q, r in zip(acc[k], outer, strip))

    lane8 = lax.broadcasted_iota(jnp.int32, (8, 128), 1)
    sub8 = lax.broadcasted_iota(jnp.int32, (8, 128), 0)

    def line_of(acc):
        table = jnp.zeros((8, 128), f32)
        for k in range(ITERS):
            total = acc[k][0] * (1.0 / DSTEP) + acc[k][1]
            table = jnp.where(sub8 == k, jnp.sum(total, axis=0, keepdims=True), table)
        line = jnp.sum(table, axis=1, keepdims=True)
        return jnp.sum(jnp.where(lane8 == sub8, line, 0.0), axis=0, keepdims=True)

    msg[...] = line_of(acc)

    slot = ident(row, col)

    def send_sums():
        for i in range(ROOTS):
            xx, yc = i // Y, i % Y * 2 + 1

            @pl.when((row != xx) | (col != yc))
            def _():
                pltpu.make_async_remote_copy(
                    msg, part.at[slot], part_send, part_recv,
                    device_id=ident(xx, yc), device_id_type=pl.DeviceIdType.LOGICAL,
                ).start()

    pl.when(jnp.logical_not(hub))(send_sums)

    lane32 = lax.broadcasted_iota(jnp.int32, (TR, 128), 1)
    for t in range(NT):
        v = xs[ITERS, t, BASE + TOP : BASE + TOP + TR, :]
        if t in (0, NT - 1):
            s = xs[ITERS, STRIP, BASE + TOP : BASE + TOP + TR, :]
            if t == 0:
                v = jnp.where(lane32 < EDGE, pltpu.roll(s, 32, 1), v)
            else:
                v = jnp.where(lane32 >= 128 - EDGE, pltpu.roll(s, 96, 1), v)
        out[:, 128 * t : 128 * t + 128] = v

    def back(c):
        return pltpu.make_async_remote_copy(
            seam_out, seam_in, back_send.at[c - (2 * Y - 1)], back_recv,
            device_id=ident(hub_row, c), device_id_type=pl.DeviceIdType.LOGICAL,
        )

    @pl.when(hub)
    def _():
        for side in (0, 1):
            for k in (-1, 0, 1):
                ref = (seam_up, seam_mid, seam_down)[k + 1]
                i = side * 3 - k + 1

                @pl.when(row_in(hub_row + k))
                def _():
                    pltpu.make_async_copy(ref.at[side], ref.at[side], seam_recv.at[i]).wait()

        fill(SEAM, [pack(ref[0], ref[1], None, None) for ref in (seam_up, seam_mid, seam_down)])
        inner = rows_in & (lane >= 32 - EDGE) & (lane < 32 + EDGE)
        seam_mask = row_mask_of(hub_row, FULL)
        seam = [sweep(k, [SEAM], FULL, seam_mask, DSTEP, lambda t, lane: inner) for k in range(ITERS)]
        seam_out[...] = xs[ITERS, SEAM, BASE + TOP : BASE + TOP + TR, :]
        msg[...] = msg[...] + line_of(seam)
        back(2 * Y - 1).start()
        back(2 * Y).start()
        send_sums()

    for here, lanes, cols in (
        (before, lane32 >= 128 - EDGE, slice(TC - 128, TC)), (after, lane32 < EDGE, slice(0, 128))
    ):

        @pl.when(here)
        def _():
            pltpu.make_async_copy(seam_in, seam_in, back_recv).wait()
            out[:, cols] = jnp.where(lanes, pltpu.roll(seam_in[...], 96, 1), out[:, cols])

    def rows_of(ref, n, sem):
        return pltpu.make_async_copy(ref.at[0:n], ref.at[0:n], sem)

    @pl.when(is_root)
    def _():
        part[slot] = msg[...]
        rows_of(part, N_ROW * N_COL - 1, part_recv).wait()
        step = N_ROW * N_COL // 16
        total = [jnp.sum(part[step * i : step * i + step], axis=0) for i in range(16)]
        while len(total) > 1:
            total = [p + q for p, q in zip(total[::2], total[1::2])]
        total = total[0]
        result[...] = total * (1.0 / CELLS)

        def tell(target):
            pltpu.make_async_remote_copy(
                result, result, result_send, result_recv, device_id=target, device_id_type=pl.DeviceIdType.LOGICAL
            ).start()

        tell(ident(row, col - 1))

        @pl.loop(1, Z)
        def _(zz):
            r, c = lax.rem(zz, Z_LO) * X + x, ((zz // Z_LO) * Y + y) * 2
            tell(ident(r, c))
            tell(ident(r, c + 1))

        gap[...] = result[...]
        rows_of(part, 2 * Z - 1, result_send).wait()
        rows_of(part, ROOTS - 1, part_send).wait()

    @pl.when(jnp.logical_not(is_root))
    def _():
        pltpu.make_async_copy(result, result, result_recv).wait()
        gap[...] = result[...]
        rows_of(part, ROOTS, part_send).wait()

    for dr, dc in SIDES:
        pl.when(exists(dr, dc))(lambda dr=dr, dc=dc: halo(dr, dc).wait_send())
    for side, here in enumerate((before, after)):
        for k in (-1, 0, 1):
            pl.when(here & row_in(row + k))(lambda side=side, k=k: to_hub(side, k).wait_send())

    @pl.when(hub)
    def _():
        back(2 * Y - 1).wait_send()
        back(2 * Y).wait_send()


def finish(denoised, line, out, gap):
    out[...] = denoised[...]
    gap[...] = line[0, :ITERS]


def on_device(noisy):
    f32 = jnp.float32
    vmem = pl.BlockSpec(memory_space=pltpu.VMEM)
    frame = lambda n: pltpu.VMEM((n, NT + 2, BUF, 128), f32)
    dma = pltpu.SemaphoreType.DMA
    denoised, gap = pl.pallas_call(
        kernel,
        out_shape=(jax.ShapeDtypeStruct((TR, TC), f32), jax.ShapeDtypeStruct((1, 128), f32)),
        in_specs=[pl.BlockSpec(memory_space=pltpu.HBM)],
        out_specs=(vmem, vmem),
        scratch_shapes=[
            pltpu.VMEM((TR, TC), f32),
            pltpu.VMEM((8, TC), f32),
            pltpu.VMEM((8, TC), f32),
            pltpu.VMEM((TR, 128), f32),
            pltpu.VMEM((TR, 128), f32),
            pltpu.VMEM((4, 8, 128), f32),
            pltpu.VMEM((2, TR, 128), f32),
            pltpu.VMEM((2, 8, 128), f32),
            pltpu.VMEM((2, 8, 128), f32),
            pltpu.VMEM((TR, 128), f32),
            pltpu.VMEM((TR, 128), f32),
            frame(ITERS + 1), frame(ITERS), frame(ITERS), frame(ITERS), frame(ITERS), frame(ITERS), frame(ITERS),
            pltpu.VMEM((1, 128), f32),
            pltpu.VMEM((N_ROW * N_COL, 1, 128), f32),
            pltpu.VMEM((1, 128), f32),
            dma, dma((8,)), dma((8,)), dma, dma, dma, dma, dma((3,)), dma((6,)), dma((2,)), dma,
        ],
        compiler_params=pltpu.CompilerParams(
            collective_id=0, has_side_effects=True, vmem_limit_bytes=24 * 1024 * 1024
        ),
    )(pltpu.with_memory_space_constraint(noisy, pltpu.HBM))
    return pl.pallas_call(
        finish,
        out_shape=(jax.ShapeDtypeStruct((TR, TC), f32), jax.ShapeDtypeStruct((ITERS,), f32)),
        in_specs=[vmem, vmem],
        out_specs=(vmem, vmem),
        compiler_params=pltpu.CompilerParams(vmem_limit_bytes=4 * 1024 * 1024),
    )(denoised, gap)


def solution(mesh):
    return jax.shard_map(
        on_device,
        mesh=mesh,
        in_specs=(P("row", "col"),),
        out_specs=(P("row", "col"), P()),
        check_vma=False,
    )
```

```python
import jax
import jax.numpy as jnp
from jax import lax
from jax.experimental import pallas as pl
from jax.experimental.pallas import tpu as pltpu
from jax.sharding import PartitionSpec as P

ITERS = 4
Z_LO, X, Z_HI, Y = 8, 4, 2, 4
Z = Z_HI * Z_LO
N_ROW, N_COL = Z_LO * X, Z_HI * Y * 2
ROOTS = [(0, 1), (0, 0), (X, 1), (X, 0)] + [(i // Y, i % Y * 2 + 1) for i in range(1, X * Y)]
N_ROOTS = len(ROOTS)
TR, TC = 32, 2048
NT = TC // 128
FR = 40
BASE = 8
BUF = 56
TOP = 4
STRIP = NT
SEAM = NT + 1
EDGE = 8

FIDELITY = 8.0
PSTEP = 0.35
DSTEP = 0.35
KA = 1.0 / (1.0 + PSTEP * FIDELITY)
KB = PSTEP / (1.0 + PSTEP * FIDELITY)
KC = PSTEP * FIDELITY / (1.0 + PSTEP * FIDELITY)
CELLS = float(N_ROW * TR * N_COL * TC)
TINY = 1e-37

SIDES = [(dr, dc) for dr in (-1, 0, 1) for dc in (-1, 0, 1) if (dr, dc) != (0, 0)]


def kernel(
    noisy, out, gap, own, top, bot, lef, rig, corners, seam_mid, seam_up, seam_down, seam_out, seam_in, xs, pr, pc, er, ec, gr, gc,
    msg, part, result, own_sem, send_sem, recv_sem, part_send, part_recv,
    result_send, result_recv, seam_send, seam_recv, back_send, back_recv,
):
    f32 = jnp.float32
    row, col = lax.axis_index("row"), lax.axis_index("col")
    zl, x = row // X, row % X
    zh, y, core = col // (2 * Y), (col // 2) % Y, col % 2
    z = zh * Z_LO + zl

    def lane_of(wins):
        return lax.broadcasted_iota(jnp.int32, (sum(n for _, n in wins), 128), 1)

    def row_of(wins):
        return jnp.concatenate([a + lax.broadcasted_iota(jnp.int32, (n, 128), 0) for a, n in wins], axis=0)

    origin = (x == 0) & (y == 0)
    is_root = ((z == 0) & ((core == 1) | origin)) | ((z == 1) & origin)
    before, after = col == 2 * Y - 1, col == 2 * Y
    hub = z == 0
    hub_row = col * X + x

    def ident(r, c):
        return r * N_COL + c

    def hub_of(r):
        return ident(r % X, r // X)

    def exists(dr, dc):
        cond = jnp.logical_not(before if dc > 0 else after) if dc else None
        for t in ([row >= 1] if dr < 0 else [row < N_ROW - 1] if dr > 0 else []) + (
            [col >= 1] if dc < 0 else [col < N_COL - 1] if dc > 0 else []
        ):
            cond = t if cond is None else cond & t
        return cond

    own_copy = pltpu.make_async_copy(noisy, own, own_sem)
    own_copy.start()

    barrier = pltpu.get_barrier_semaphore()

    def signal(target):
        pl.semaphore_signal(barrier, inc=1, device_id=target, device_id_type=pl.DeviceIdType.LOGICAL)

    heard = []
    for dr, dc in SIDES:
        pl.when(exists(dr, dc))(lambda dr=dr, dc=dc: signal(ident(row + dr, col + dc)))
        heard.append(exists(dr, dc))

    def row_in(r):
        return (r >= 0) & (r < N_ROW)

    for k in (-1, 0, 1):
        for c in (2 * Y - 1, 2 * Y):
            pl.when(hub & row_in(hub_row + k))(lambda k=k, c=c: signal(ident(hub_row + k, c)))
        heard.append((before | after) & row_in(row + k))

    @pl.when(is_root)
    def _():
        @pl.loop(0, Z - 1)
        def _(i):
            step = (i + 1) // 2
            zz = (z + jnp.where(i % 2 == 1, Z // 2 - step, Z // 2 + step)) % Z
            for xx in range(X):
                for yc in range(2 * Y):
                    signal(ident((zz % Z_LO) * X + xx, (zz // Z_LO) * 2 * Y + yc))

        for xx in range(X):
            for yc in range(2 * Y):
                pl.when((x != xx) | (y * 2 + core != yc))(lambda xx=xx, yc=yc: signal(ident(zl * X + xx, zh * 2 * Y + yc)))

    gone = (
        (row == 0, top), (row == N_ROW - 1, bot), ((col == 0) | after, lef), ((col == N_COL - 1) | before, rig),
        (hub & (hub_row == 0), seam_up), (hub & (hub_row == N_ROW - 1), seam_down),
    )
    for cond, buf in gone:

        @pl.when(cond)
        def _():
            buf[...] = jnp.zeros_like(buf)

    for i, (dr, dc) in enumerate([(-1, -1), (-1, 1), (1, -1), (1, 1)]):

        @pl.when(jnp.logical_not(exists(dr, dc)))
        def _():
            corners[i] = jnp.zeros((8, 128), f32)

    for k in range(ITERS):
        for t in range(NT + 2):
            pr[k, t, 0:BASE, :] = jnp.zeros((BASE, 128), f32)

    own_copy.wait()
    count = jnp.where(is_root, N_ROOTS - 1, N_ROOTS)
    for hear in heard:
        count = count + jnp.where(hear, 1, 0)
    pl.semaphore_wait(barrier, count)

    place0 = {
        (-1, 0): top, (1, 0): bot, (0, -1): lef, (0, 1): rig, (-1, -1): corners.at[0], (-1, 1): corners.at[1],
        (1, -1): corners.at[2], (1, 1): corners.at[3],
    }

    place = {k: (v if k[0] == 0 else v.at[4:8] if k[0] < 0 else v.at[0:5]) for k, v in place0.items()}

    def source(dr, dc):
        rs = slice(0, TR) if dr == 0 else slice(0, 5) if dr < 0 else slice(TR - 4, TR)
        cs = slice(0, TC) if dc == 0 else slice(0, 128) if dc < 0 else slice(TC - 128, TC)
        return own.at[rs, cs]

    def halo(dr, dc):
        i = SIDES.index((dr, dc))
        return pltpu.make_async_remote_copy(
            source(dr, dc), place[(-dr, -dc)], send_sem.at[i], recv_sem.at[SIDES.index((-dr, -dc))],
            device_id=ident(row + dr, col + dc), device_id_type=pl.DeviceIdType.LOGICAL,
        )

    def arrived(dr, dc):
        i = SIDES.index((dr, dc))
        return pltpu.make_async_remote_copy(
            source(-dr, -dc), place[(dr, dc)], send_sem.at[i], recv_sem.at[i],
            device_id=ident(row, col), device_id_type=pl.DeviceIdType.LOGICAL,
        )

    for dr, dc in [(1, 0), (-1, 0), (0, 1), (0, -1), (1, 1), (1, -1), (-1, 1), (-1, -1)]:
        pl.when(exists(dr, dc))(lambda dr=dr, dc=dc: halo(dr, dc).start())

    def to_hub(side, k):
        ref = (seam_down, seam_mid, seam_up)[k + 1]
        rs = (slice(0, 8), slice(0, TR), slice(TR - 8, TR))[k + 1]
        cs = (slice(TC - 128, TC), slice(0, 128))[side]
        i = side * 3 + k + 1
        return pltpu.make_async_remote_copy(
            own.at[rs, cs], ref.at[side], seam_send.at[k + 1], seam_recv.at[i],
            device_id=hub_of(row + k), device_id_type=pl.DeviceIdType.LOGICAL,
        )

    for side, here in enumerate((before, after)):
        for k in (0, -1, 1):
            pl.when(here & row_in(row + k))(lambda side=side, k=k: to_hub(side, k).start())

    def row_mask_of(r, wins):
        grow = r * TR - TOP + row_of(wins)
        return jnp.where((grow >= 0) & (grow < N_ROW * TR - 1), DSTEP, 0.0).astype(f32)

    def load(ref, k, t, wins, shift=0):
        return jnp.concatenate([ref[k, t, BASE + a + shift : BASE + a + shift + n, :] for a, n in wins], axis=0)

    def store(ref, k, t, wins, v):
        at = 0
        for a, n in wins:
            ref[k, t, BASE + a : BASE + a + n, :] = v[at : at + n]
            at += n

    def left_of(v):
        return pltpu.roll(v, 1, 1)

    def right_of(v):
        return pltpu.roll(v, 127, 1)

    def sums(cell):
        acc = cell[0:8]
        for i in range(1, cell.shape[0] // 8):
            acc = acc + cell[8 * i : 8 * i + 8]
        return acc

    def sweep(k, tiles, wins, row_mask, col_mask, keep):
        a_sum = b_sum = prev_pc = pend = rolled_n = None
        lane = lane_of(wins)
        for t in tiles + [None]:
            if t is not None:
                n = load(xs, 0, t, wins)
                if k == 0:
                    ncol = right_of(n) if rolled_n is None else rolled_n
                    nright = ncol
                    if t != tiles[-1]:
                        rolled_n = right_of(load(xs, 0, t + 1, wins))
                        nright = jnp.where(lane == 127, rolled_n, ncol)
                    qr = (load(xs, 0, t, wins, 1) - n) * row_mask
                    qc = (nright - n) * col_mask
                    store(gr, 0, t, wins, qr)
                    store(gc, 0, t, wins, qc)
                else:
                    qr = load(pr, k - 1, t, wins) + load(er, k - 1, t, wins)
                    qc = load(pc, k - 1, t, wins) + load(ec, k - 1, t, wins)
                shrink = lax.rsqrt(jnp.maximum(qr * qr + qc * qc, 1.0))
                p_r = qr * shrink
                p_c = qc * shrink
                store(pr, k, t, wins, p_r)
                if k < ITERS - 1:
                    store(pc, k, t, wins, p_c)
                rolled = left_of(p_c)
                pleft = rolled if prev_pc is None else jnp.where(lane == 0, prev_pc, rolled)
                prev_pc = rolled
                d = (p_r - load(pr, k, t, wins, -1)) + (p_c - pleft)
                if k == 0:
                    new = n + KB * d
                else:
                    new = KA * load(xs, k, t, wins) + (KB * d + KC * n)
                store(xs, k + 1, t, wins, new)
                rolled_x = right_of(new)
            if pend is not None:
                s, sx, sd, sn, srolled = pend
                xright = srolled if t is None else jnp.where(lane == 127, rolled_x, srolled)
                g_r = (load(xs, k + 1, s, wins, 1) - sx) * row_mask
                g_c = (xright - sx) * col_mask
                if k < ITERS - 1:
                    store(er, k, s, wins, g_r + (g_r - load(gr, k, s, wins)))
                    store(ec, k, s, wins, g_c + (g_c - load(gc, k, s, wins)))
                if k < ITERS - 2:
                    store(gr, k + 1, s, wins, g_r)
                    store(gc, k + 1, s, wins, g_c)
                m = g_r * g_r + g_c * g_c
                size = m * lax.rsqrt(jnp.maximum(m, TINY))
                diff = sx - sn
                rest = (diff * diff) * (0.5 * FIDELITY) + sd * (sn + sd * (0.5 / FIDELITY))
                mask = keep(s, lane)
                size = sums(jnp.where(mask, size, 0.0))
                rest = sums(jnp.where(mask, rest, 0.0))
                a_sum = size if a_sum is None else a_sum + size
                b_sum = rest if b_sum is None else b_sum + rest
            if t is not None:
                pend = (t, new, d, n, rolled_x)
        return a_sum, b_sum

    def wait_side(dr, dc):
        pl.when(exists(dr, dc))(lambda: arrived(dr, dc).wait_recv())

    def columns(t, lane):
        if t == 0:
            return lane >= EDGE
        if t == NT - 1:
            return lane < 128 - EDGE
        return None

    def keep_rows(wins, first, last):
        a = row_of(wins)
        inside = (a >= TOP + first) & (a <= TOP + last)

        def keep(t, lane):
            here = columns(t, lane)
            return inside if here is None else inside & here

        return keep

    MAIN = list(range(NT))
    FULL = [(0, FR)]
    INNER = [(TOP, TR)]
    for t in MAIN:
        xs[0, t, BASE + TOP : BASE + TOP + TR, :] = own[:, 128 * t : 128 * t + 128]
    inner_mask = row_mask_of(row, INNER)
    acc = []
    for k in range(ITERS):
        acc.append(sweep(k, MAIN, INNER, inner_mask, DSTEP, keep_rows(INNER, k + 1, TR - 3 - k)))

    wait_side(-1, 0)
    wait_side(1, 0)
    for dr in (-1, 0, 1):
        wait_side(dr, -1)
        wait_side(dr, 1)
    for t in MAIN:
        cs = slice(128 * t, 128 * t + 128)
        xs[0, t, BASE + TOP - 8 : BASE + TOP, :] = top[:, cs]
        xs[0, t, BASE + TOP + TR : BASE + TOP + TR + 8, :] = bot[:, cs]

    def pack(last, right, left, first):
        q = lax.broadcasted_iota(jnp.int32, last.shape, 1)
        v = jnp.where(q < 32, pltpu.roll(last, 32, 1), pltpu.roll(right, 32, 1))
        if left is None:
            return v
        w = jnp.where(q < 96, pltpu.roll(left, 96, 1), pltpu.roll(first, 96, 1))
        return jnp.where(q < 64, v, w)

    def fill(t, parts):
        xs[0, t, BASE + TOP - 8 : BASE + TOP, :] = parts[0]
        xs[0, t, BASE + TOP : BASE + TOP + TR, :] = parts[1]
        xs[0, t, BASE + TOP + TR : BASE + TOP + TR + 8, :] = parts[2]

    lo, hi = slice(0, 128), slice(TC - 128, TC)
    fill(STRIP, [
        pack(top[:, hi], corners[1], corners[0], top[:, lo]),
        pack(own[:, hi], rig[...], lef[...], own[:, lo]),
        pack(bot[:, hi], corners[3], corners[2], bot[:, lo]),
    ])
    lane = lane_of(FULL)
    outside = ((col == 0) & (lane >= 64) & (lane < 96)) | ((col == N_COL - 1) & (lane >= 31) & (lane < 64))
    strip_mask = jnp.where(outside, 0.0, DSTEP).astype(f32)
    rows_in = (row_of(FULL) >= TOP) & (row_of(FULL) < TOP + TR)
    owned = jnp.logical_not(before) & (lane >= 32 - EDGE) & (lane < 32)
    owned = owned | (jnp.logical_not(after) & (lane >= 96) & (lane < 96 + EDGE))
    owned = owned & rows_in
    full_mask = row_mask_of(row, FULL)
    for k in range(ITERS):
        wins = [(k, 8), (32 - k, 8)]
        rows = row_of(wins)
        edge = ((rows >= TOP) & (rows <= TOP + k)) | ((rows >= TOP + TR - 2 - k) & (rows < TOP + TR))

        def keep(t, lane, edge=edge):
            here = columns(t, lane)
            return edge if here is None else edge & here

        outer = sweep(k, MAIN, wins, row_mask_of(row, wins), DSTEP, keep)
        strip = sweep(k, [STRIP], FULL, full_mask, strip_mask, lambda t, lane: owned)
        acc[k] = tuple(p + q + r for p, q, r in zip(acc[k], outer, strip))

    lane8 = lax.broadcasted_iota(jnp.int32, (8, 128), 1)

    def line_of(acc):
        table = jnp.zeros((8, 128), f32)
        for k in range(ITERS):
            total = acc[k][0] * (1.0 / DSTEP) + acc[k][1]
            table = jnp.where(lane8 == k, jnp.sum(total, axis=1, keepdims=True), table)
        return jnp.sum(table, axis=0, keepdims=True)

    msg[...] = line_of(acc)

    slot = ident(row, col)

    def send_sums():
        for xx, yc in ROOTS:

            @pl.when((row != xx) | (col != yc))
            def _():
                pltpu.make_async_remote_copy(
                    msg, part.at[slot], part_send, part_recv,
                    device_id=ident(xx, yc), device_id_type=pl.DeviceIdType.LOGICAL,
                ).start()

    pl.when(jnp.logical_not(hub))(send_sums)

    lane32 = lax.broadcasted_iota(jnp.int32, (TR, 128), 1)
    for t in range(NT):
        v = xs[ITERS, t, BASE + TOP : BASE + TOP + TR, :]
        if t in (0, NT - 1):
            s = xs[ITERS, STRIP, BASE + TOP : BASE + TOP + TR, :]
            if t == 0:
                v = jnp.where(lane32 < EDGE, pltpu.roll(s, 32, 1), v)
            else:
                v = jnp.where(lane32 >= 128 - EDGE, pltpu.roll(s, 96, 1), v)
        out[:, 128 * t : 128 * t + 128] = v

    def back(c):
        return pltpu.make_async_remote_copy(
            seam_out, seam_in, back_send.at[c - (2 * Y - 1)], back_recv,
            device_id=ident(hub_row, c), device_id_type=pl.DeviceIdType.LOGICAL,
        )

    @pl.when(hub)
    def _():
        for side in (0, 1):
            for k in (-1, 0, 1):
                ref = (seam_up, seam_mid, seam_down)[k + 1]
                i = side * 3 - k + 1

                @pl.when(row_in(hub_row + k))
                def _():
                    pltpu.make_async_copy(ref.at[side], ref.at[side], seam_recv.at[i]).wait()

        fill(SEAM, [pack(ref[0], ref[1], None, None) for ref in (seam_up, seam_mid, seam_down)])
        inner = rows_in & (lane >= 32 - EDGE) & (lane < 32 + EDGE)
        seam_mask = row_mask_of(hub_row, FULL)
        seam = [sweep(k, [SEAM], FULL, seam_mask, DSTEP, lambda t, lane: inner) for k in range(ITERS)]
        seam_out[...] = xs[ITERS, SEAM, BASE + TOP : BASE + TOP + TR, :]
        msg[...] = msg[...] + line_of(seam)
        back(2 * Y - 1).start()
        back(2 * Y).start()
        send_sums()

    for here, lanes, cols in (
        (before, lane32 >= 128 - EDGE, slice(TC - 128, TC)), (after, lane32 < EDGE, slice(0, 128))
    ):

        @pl.when(here)
        def _():
            pltpu.make_async_copy(seam_in, seam_in, back_recv).wait()
            out[:, cols] = jnp.where(lanes, pltpu.roll(seam_in[...], 96, 1), out[:, cols])

    def rows_of(ref, n, sem):
        return pltpu.make_async_copy(ref.at[0:n], ref.at[0:n], sem)

    @pl.when(is_root)
    def _():
        part[slot] = msg[...]
        rows_of(part, N_ROW * N_COL - 1, part_recv).wait()
        step = N_ROW * N_COL // 16
        total = [jnp.sum(part[step * i : step * i + step], axis=0) for i in range(16)]
        while len(total) > 1:
            total = [p + q for p, q in zip(total[::2], total[1::2])]
        total = total[0]
        result[...] = total * (1.0 / CELLS)

        def tell(target):
            pltpu.make_async_remote_copy(
                result, result, result_send, result_recv, device_id=target, device_id_type=pl.DeviceIdType.LOGICAL
            ).start()

        gap[...] = result[...]

        def tell_planes(start, stop):
            @pl.loop(start, stop)
            def _(zz):
                r, c = lax.rem(zz, Z_LO) * X + x, ((zz // Z_LO) * Y + y) * 2
                tell(ident(r, c))
                tell(ident(r, c + 1))

            rows_of(part, 2 * (stop - start), result_send).wait()

        pl.when(hub & (core == 0))(lambda: tell_planes(2, Z))

        @pl.when(hub & (core == 1) & jnp.logical_not(origin))
        def _():
            tell(ident(row, col - 1))
            tell_planes(1, Z)
            rows_of(part, 1, result_send).wait()

        rows_of(part, N_ROOTS - 1, part_send).wait()

    @pl.when(jnp.logical_not(is_root))
    def _():
        pltpu.make_async_copy(result, result, result_recv).wait()
        gap[...] = result[...]
        rows_of(part, N_ROOTS, part_send).wait()

    for dr, dc in SIDES:
        pl.when(exists(dr, dc))(lambda dr=dr, dc=dc: halo(dr, dc).wait_send())
    for side, here in enumerate((before, after)):
        for k in (-1, 0, 1):
            pl.when(here & row_in(row + k))(lambda side=side, k=k: to_hub(side, k).wait_send())

    @pl.when(hub)
    def _():
        back(2 * Y - 1).wait_send()
        back(2 * Y).wait_send()


def finish(denoised, line, out, gap):
    out[...] = denoised[...]
    gap[...] = line[0, :ITERS]


def on_device(noisy):
    f32 = jnp.float32
    vmem = pl.BlockSpec(memory_space=pltpu.VMEM)
    frame = lambda n: pltpu.VMEM((n, NT + 2, BUF, 128), f32)
    dma = pltpu.SemaphoreType.DMA
    denoised, gap = pl.pallas_call(
        kernel,
        out_shape=(jax.ShapeDtypeStruct((TR, TC), f32), jax.ShapeDtypeStruct((1, 128), f32)),
        in_specs=[pl.BlockSpec(memory_space=pltpu.HBM)],
        out_specs=(vmem, vmem),
        scratch_shapes=[
            pltpu.VMEM((TR, TC), f32),
            pltpu.VMEM((8, TC), f32),
            pltpu.VMEM((8, TC), f32),
            pltpu.VMEM((TR, 128), f32),
            pltpu.VMEM((TR, 128), f32),
            pltpu.VMEM((4, 8, 128), f32),
            pltpu.VMEM((2, TR, 128), f32),
            pltpu.VMEM((2, 8, 128), f32),
            pltpu.VMEM((2, 8, 128), f32),
            pltpu.VMEM((TR, 128), f32),
            pltpu.VMEM((TR, 128), f32),
            frame(ITERS + 1), frame(ITERS), frame(ITERS), frame(ITERS), frame(ITERS), frame(ITERS), frame(ITERS),
            pltpu.VMEM((1, 128), f32),
            pltpu.VMEM((N_ROW * N_COL, 1, 128), f32),
            pltpu.VMEM((1, 128), f32),
            dma, dma((8,)), dma((8,)), dma, dma, dma, dma, dma((3,)), dma((6,)), dma((2,)), dma,
        ],
        compiler_params=pltpu.CompilerParams(
            collective_id=0, has_side_effects=True, vmem_limit_bytes=24 * 1024 * 1024
        ),
    )(pltpu.with_memory_space_constraint(noisy, pltpu.HBM))
    return pl.pallas_call(
        finish,
        out_shape=(jax.ShapeDtypeStruct((TR, TC), f32), jax.ShapeDtypeStruct((ITERS,), f32)),
        in_specs=[vmem, vmem],
        out_specs=(vmem, vmem),
        compiler_params=pltpu.CompilerParams(vmem_limit_bytes=4 * 1024 * 1024),
    )(denoised, gap)


def solution(mesh):
    return jax.shard_map(
        on_device,
        mesh=mesh,
        in_specs=(P("row", "col"),),
        out_specs=(P("row", "col"), P()),
        check_vma=False,
    )
```

```python
import jax
import jax.numpy as jnp
from jax import lax
from jax.experimental import pallas as pl
from jax.experimental.pallas import tpu as pltpu
from jax.sharding import PartitionSpec as P

ITERS = 4
Z_LO, X, Z_HI, Y = 8, 4, 2, 4
Z = Z_HI * Z_LO
N_ROW, N_COL = Z_LO * X, Z_HI * Y * 2
ALONE = 2
ROOTS = [(0, 1), (0, 0)] + [(X * i, c) for i in range(1, ALONE + 1) for c in (1, 0)]
ROOTS += [(i // Y, i % Y * 2 + 1) for i in range(1, X * Y)]
N_ROOTS = len(ROOTS)
TR, TC = 32, 2048
NT = TC // 128
FR = 40
BASE = 8
BUF = 56
TOP = 4
STRIP = NT
SEAM = NT + 1
EDGE = 8

FIDELITY = 8.0
PSTEP = 0.35
DSTEP = 0.35
KA = 1.0 / (1.0 + PSTEP * FIDELITY)
KB = PSTEP / (1.0 + PSTEP * FIDELITY)
KC = PSTEP * FIDELITY / (1.0 + PSTEP * FIDELITY)
CELLS = float(N_ROW * TR * N_COL * TC)
TINY = 1e-37
INNER_SKEW = 20
SKEW = 4

SIDES = [(dr, dc) for dr in (-1, 0, 1) for dc in (-1, 0, 1) if (dr, dc) != (0, 0)]


def kernel(
    noisy, out, gap, own, top, bot, lef, rig, corners, seam_mid, seam_up, seam_down, seam_out, seam_in, xs, nc, pr, pc, er, ec, gr, gc,
    msg, part, result, own_sem, send_sem, recv_sem, part_send, part_recv,
    result_send, result_recv, seam_send, seam_recv, back_send, back_recv,
):
    f32 = jnp.float32
    row, col = lax.axis_index("row"), lax.axis_index("col")
    zl, x = row // X, row % X
    zh, y, core = col // (2 * Y), (col // 2) % Y, col % 2
    z = zh * Z_LO + zl

    def lane_of(wins):
        return lax.broadcasted_iota(jnp.int32, (sum(n for _, n in wins), 128), 1)

    def row_of(wins):
        return jnp.concatenate([a + lax.broadcasted_iota(jnp.int32, (n, 128), 0) for a, n in wins], axis=0)

    origin = (x == 0) & (y == 0)
    is_root = ((z == 0) & ((core == 1) | origin)) | ((z >= 1) & (z <= ALONE) & origin)
    before, after = col == 2 * Y - 1, col == 2 * Y
    hub = z == 0
    hub_row = col * X + x

    def ident(r, c):
        return r * N_COL + c

    def hub_of(r):
        return ident(r % X, r // X)

    def exists(dr, dc):
        cond = jnp.logical_not(before if dc > 0 else after) if dc else None
        for t in ([row >= 1] if dr < 0 else [row < N_ROW - 1] if dr > 0 else []) + (
            [col >= 1] if dc < 0 else [col < N_COL - 1] if dc > 0 else []
        ):
            cond = t if cond is None else cond & t
        return cond

    own_copies = [
        pltpu.make_async_copy(noisy.at[8 * i : 8 * i + 8], own.at[8 * i : 8 * i + 8], own_sem.at[i])
        for i in range(TR // 8)
    ]
    for i in (0, 3, 1, 2):
        own_copies[i].start()

    barrier = pltpu.get_barrier_semaphore()

    def signal(target):
        pl.semaphore_signal(barrier, inc=1, device_id=target, device_id_type=pl.DeviceIdType.LOGICAL)

    heard = []
    for dr, dc in SIDES:
        pl.when(exists(dr, dc))(lambda dr=dr, dc=dc: signal(ident(row + dr, col + dc)))
        heard.append(exists(dr, dc))

    def row_in(r):
        return (r >= 0) & (r < N_ROW)

    for k in (-1, 0, 1):
        for c in (2 * Y - 1, 2 * Y):
            pl.when(hub & row_in(hub_row + k))(lambda k=k, c=c: signal(ident(hub_row + k, c)))
        heard.append((before | after) & row_in(row + k))

    @pl.when(is_root)
    def _():
        @pl.loop(0, Z - 1)
        def _(i):
            step = (i + 1) // 2
            zz = (z + jnp.where(i % 2 == 1, Z // 2 - step, Z // 2 + step)) % Z
            for xx in range(X):
                for yc in range(2 * Y):
                    signal(ident((zz % Z_LO) * X + xx, (zz // Z_LO) * 2 * Y + yc))

        for xx in range(X):
            for yc in range(2 * Y):
                pl.when((x != xx) | (y * 2 + core != yc))(lambda xx=xx, yc=yc: signal(ident(zl * X + xx, zh * 2 * Y + yc)))

    gone = (
        (row == 0, top), (row == N_ROW - 1, bot), ((col == 0) | after, lef), ((col == N_COL - 1) | before, rig),
        (hub & (hub_row == 0), seam_up), (hub & (hub_row == N_ROW - 1), seam_down),
    )
    for cond, buf in gone:

        @pl.when(cond)
        def _():
            buf[...] = jnp.zeros_like(buf)

    for i, (dr, dc) in enumerate([(-1, -1), (-1, 1), (1, -1), (1, 1)]):

        @pl.when(jnp.logical_not(exists(dr, dc)))
        def _():
            corners[i] = jnp.zeros((8, 128), f32)

    for k in range(ITERS):
        for t in range(NT + 2):
            pr[k, t, 0:BASE, :] = jnp.zeros((BASE, 128), f32)

    own_copies[0].wait()
    own_copies[3].wait()
    count = jnp.where(is_root, N_ROOTS - 1, N_ROOTS)
    for hear in heard:
        count = count + jnp.where(hear, 1, 0)
    pl.semaphore_wait(barrier, count)

    place0 = {
        (-1, 0): top, (1, 0): bot, (0, -1): lef, (0, 1): rig, (-1, -1): corners.at[0], (-1, 1): corners.at[1],
        (1, -1): corners.at[2], (1, 1): corners.at[3],
    }

    place = {k: (v if k[0] == 0 else v.at[4:8] if k[0] < 0 else v.at[0:5]) for k, v in place0.items()}

    def source(dr, dc):
        rs = slice(0, TR) if dr == 0 else slice(0, 5) if dr < 0 else slice(TR - 4, TR)
        cs = slice(0, TC) if dc == 0 else slice(0, 128) if dc < 0 else slice(TC - 128, TC)
        return own.at[rs, cs]

    def halo(dr, dc):
        i = SIDES.index((dr, dc))
        return pltpu.make_async_remote_copy(
            source(dr, dc), place[(-dr, -dc)], send_sem.at[i], recv_sem.at[SIDES.index((-dr, -dc))],
            device_id=ident(row + dr, col + dc), device_id_type=pl.DeviceIdType.LOGICAL,
        )

    def arrived(dr, dc):
        i = SIDES.index((dr, dc))
        return pltpu.make_async_remote_copy(
            source(-dr, -dc), place[(dr, dc)], send_sem.at[i], recv_sem.at[i],
            device_id=ident(row, col), device_id_type=pl.DeviceIdType.LOGICAL,
        )

    for dr, dc in [(1, 1), (1, -1), (-1, 1), (-1, -1), (1, 0), (-1, 0), (0, 1), (0, -1)]:
        if (dr, dc) == (0, 1):
            own_copies[1].wait()
            own_copies[2].wait()
        pl.when(exists(dr, dc))(lambda dr=dr, dc=dc: halo(dr, dc).start())

    def to_hub(side, k):
        ref = (seam_down, seam_mid, seam_up)[k + 1]
        rs = (slice(0, 8), slice(0, TR), slice(TR - 8, TR))[k + 1]
        cs = (slice(TC - 128, TC), slice(0, 128))[side]
        i = side * 3 + k + 1
        return pltpu.make_async_remote_copy(
            own.at[rs, cs], ref.at[side], seam_send.at[k + 1], seam_recv.at[i],
            device_id=hub_of(row + k), device_id_type=pl.DeviceIdType.LOGICAL,
        )

    for side, here in enumerate((before, after)):
        for k in (0, -1, 1):
            pl.when(here & row_in(row + k))(lambda side=side, k=k: to_hub(side, k).start())

    def row_mask_of(r, wins):
        grow = r * TR - TOP + row_of(wins)
        return jnp.where((grow >= 0) & (grow < N_ROW * TR - 1), 1.0, 0.0).astype(f32)

    def load(ref, k, t, wins, shift=0):
        return jnp.concatenate([ref[k, t, BASE + a + shift : BASE + a + shift + n, :] for a, n in wins], axis=0)

    def store(ref, k, t, wins, v):
        at = 0
        for a, n in wins:
            ref[k, t, BASE + a : BASE + a + n, :] = v[at : at + n]
            at += n

    def left_of(v):
        return pltpu.roll(v, 1, 1)

    def right_of(v):
        return pltpu.roll(v, 127, 1)

    def sums(cell):
        acc = cell[0:8]
        for i in range(1, cell.shape[0] // 8):
            acc = acc + cell[8 * i : 8 * i + 8]
        return acc

    def sweep(k, tiles, wins, row_mask, col_mask, keep):
        def masked(v, mask):
            return v if mask is None else v * mask

        total = prev_pc = pend = rolled_n = None
        lane = lane_of(wins)
        for t in tiles + [None]:
            if t is not None:
                n = load(xs, 0, t, wins)
                if k == 0:
                    ncol = right_of(n) if rolled_n is None else rolled_n
                    nright = ncol
                    if t != tiles[-1]:
                        rolled_n = right_of(load(xs, 0, t + 1, wins))
                        nright = jnp.where(lane == 127, rolled_n, ncol)
                    qr = masked(load(xs, 0, t, wins, 1) - n, row_mask)
                    qc = masked(nright - n, col_mask)
                    store(gr, 0, t, wins, qr)
                    store(gc, 0, t, wins, qc)
                else:
                    qr = load(pr, k - 1, t, wins) + load(er, k - 1, t, wins)
                    qc = load(pc, k - 1, t, wins) + load(ec, k - 1, t, wins)
                shrink = lax.rsqrt(jnp.maximum(qr * qr + qc * qc, 1.0))
                p_r = qr * shrink
                p_c = qc * shrink
                store(pr, k, t, wins, p_r)
                if k < ITERS - 1:
                    store(pc, k, t, wins, p_c)
                rolled = left_of(p_c)
                pleft = rolled if prev_pc is None else jnp.where(lane == 0, prev_pc, rolled)
                prev_pc = rolled
                d = (p_r - load(pr, k, t, wins, -1)) + (p_c - pleft)
                if k == 0:
                    new = n + (KB * DSTEP) * d
                    store(nc, 0, t, wins, n * KC)
                else:
                    new = KA * load(xs, k, t, wins) + ((KB * DSTEP) * d + load(nc, 0, t, wins))
                store(xs, k + 1, t, wins, new)
                rolled_x = right_of(new)
            if pend is not None:
                s, sx, sd, sn, srolled = pend
                xright = srolled if t is None else jnp.where(lane == 127, rolled_x, srolled)
                g_r = masked(load(xs, k + 1, s, wins, 1) - sx, row_mask)
                g_c = masked(xright - sx, col_mask)
                if k < ITERS - 1:
                    store(er, k, s, wins, g_r + (g_r - load(gr, k, s, wins)))
                    store(ec, k, s, wins, g_c + (g_c - load(gc, k, s, wins)))
                if k < ITERS - 2:
                    store(gr, k + 1, s, wins, g_r)
                    store(gc, k + 1, s, wins, g_c)
                m = g_r * g_r + g_c * g_c
                size = m * lax.rsqrt(jnp.maximum(m, TINY))
                diff = sx - sn
                cell = (diff * diff) * (0.5 * FIDELITY / DSTEP) + sd * (sn + sd * (0.5 * DSTEP / FIDELITY))
                cell = sums(jnp.where(keep(s, lane), cell + size, 0.0))
                total = cell if total is None else total + cell
            if t is not None:
                pend = (t, new, d, n, rolled_x)
            yield
        return total

    def interleave(work):
        work = [list(w) for w in work]
        results = [None] * len(work)
        step = 0
        while any(g is not None for _, g in work):
            for i, (start, g) in enumerate(work):
                if g is not None and step >= start:
                    try:
                        next(g)
                    except StopIteration as end:
                        results[i] = end.value
                        work[i][1] = None
            step += 1
        return results

    def wait_side(dr, dc):
        pl.when(exists(dr, dc))(lambda: arrived(dr, dc).wait_recv())

    def columns(t, lane):
        if t == 0:
            return lane >= EDGE
        if t == NT - 1:
            return lane < 128 - EDGE
        return None

    def keep_rows(wins, first, last):
        a = row_of(wins)
        inside = (a >= TOP + first) & (a <= TOP + last)

        def keep(t, lane):
            here = columns(t, lane)
            return inside if here is None else inside & here

        return keep

    MAIN = list(range(NT))
    FULL = [(0, FR)]
    INNER = [(TOP, TR)]
    for t in MAIN:
        xs[0, t, BASE + TOP : BASE + TOP + TR, :] = own[:, 128 * t : 128 * t + 128] * DSTEP
    acc = interleave(
        (k * INNER_SKEW, sweep(k, MAIN, INNER, None, None, keep_rows(INNER, k + 1, TR - 3 - k)))
        for k in range(ITERS)
    )

    wait_side(-1, 0)
    wait_side(1, 0)
    for dr in (-1, 0, 1):
        wait_side(dr, -1)
        wait_side(dr, 1)
    for t in MAIN:
        cs = slice(128 * t, 128 * t + 128)
        xs[0, t, BASE + TOP - 8 : BASE + TOP, :] = top[:, cs] * DSTEP
        xs[0, t, BASE + TOP + TR : BASE + TOP + TR + 8, :] = bot[:, cs] * DSTEP

    def pack(last, right, left, first):
        q = lax.broadcasted_iota(jnp.int32, last.shape, 1)
        v = jnp.where(q < 32, pltpu.roll(last, 32, 1), pltpu.roll(right, 32, 1))
        if left is None:
            return v
        w = jnp.where(q < 96, pltpu.roll(left, 96, 1), pltpu.roll(first, 96, 1))
        return jnp.where(q < 64, v, w)

    def fill(t, parts):
        xs[0, t, BASE + TOP - 8 : BASE + TOP, :] = parts[0] * DSTEP
        xs[0, t, BASE + TOP : BASE + TOP + TR, :] = parts[1] * DSTEP
        xs[0, t, BASE + TOP + TR : BASE + TOP + TR + 8, :] = parts[2] * DSTEP

    lo, hi = slice(0, 128), slice(TC - 128, TC)
    fill(STRIP, [
        pack(top[:, hi], corners[1], corners[0], top[:, lo]),
        pack(own[:, hi], rig[...], lef[...], own[:, lo]),
        pack(bot[:, hi], corners[3], corners[2], bot[:, lo]),
    ])
    lane = lane_of(FULL)
    outside = ((col == 0) & (lane >= 64) & (lane < 96)) | ((col == N_COL - 1) & (lane >= 31) & (lane < 64))
    strip_mask = jnp.where(outside, 0.0, 1.0).astype(f32)
    rows_in = (row_of(FULL) >= TOP) & (row_of(FULL) < TOP + TR)
    owned = jnp.logical_not(before) & (lane >= 32 - EDGE) & (lane < 32)
    owned = owned | (jnp.logical_not(after) & (lane >= 96) & (lane < 96 + EDGE))
    owned = owned & rows_in
    full_mask = row_mask_of(row, FULL)
    work = []
    for k in range(ITERS):
        wins = [(k, 8), (32 - k, 8)]
        rows = row_of(wins)
        edge = ((rows >= TOP) & (rows <= TOP + k)) | ((rows >= TOP + TR - 2 - k) & (rows < TOP + TR))

        def keep(t, lane, edge=edge):
            here = columns(t, lane)
            return edge if here is None else edge & here

        work.append((k * SKEW, sweep(k, MAIN, wins, row_mask_of(row, wins), None, keep)))
        work.append((k * SKEW, sweep(k, [STRIP], FULL, full_mask, strip_mask, lambda t, lane: owned)))
    done = interleave(work)
    acc = [acc[k] + done[2 * k] + done[2 * k + 1] for k in range(ITERS)]

    lane8 = lax.broadcasted_iota(jnp.int32, (8, 128), 1)

    def line_of(acc):
        table = jnp.zeros((8, 128), f32)
        for k in range(ITERS):
            table = jnp.where(lane8 == k, jnp.sum(acc[k], axis=1, keepdims=True), table)
        return jnp.sum(table, axis=0, keepdims=True)

    msg[...] = line_of(acc)

    slot = ident(row, col)

    def send_sums():
        for xx, yc in ROOTS:

            @pl.when((row != xx) | (col != yc))
            def _():
                pltpu.make_async_remote_copy(
                    msg, part.at[slot], part_send, part_recv,
                    device_id=ident(xx, yc), device_id_type=pl.DeviceIdType.LOGICAL,
                ).start()

    pl.when(jnp.logical_not(hub))(send_sums)

    lane32 = lax.broadcasted_iota(jnp.int32, (TR, 128), 1)
    for t in range(NT):
        v = xs[ITERS, t, BASE + TOP : BASE + TOP + TR, :]
        if t in (0, NT - 1):
            s = xs[ITERS, STRIP, BASE + TOP : BASE + TOP + TR, :]
            if t == 0:
                v = jnp.where(lane32 < EDGE, pltpu.roll(s, 32, 1), v)
            else:
                v = jnp.where(lane32 >= 128 - EDGE, pltpu.roll(s, 96, 1), v)
        out[:, 128 * t : 128 * t + 128] = v * (1.0 / DSTEP)

    def back(c):
        return pltpu.make_async_remote_copy(
            seam_out, seam_in, back_send.at[c - (2 * Y - 1)], back_recv,
            device_id=ident(hub_row, c), device_id_type=pl.DeviceIdType.LOGICAL,
        )

    @pl.when(hub)
    def _():
        for side in (0, 1):
            for k in (-1, 0, 1):
                ref = (seam_up, seam_mid, seam_down)[k + 1]
                i = side * 3 - k + 1

                @pl.when(row_in(hub_row + k))
                def _():
                    pltpu.make_async_copy(ref.at[side], ref.at[side], seam_recv.at[i]).wait()

        fill(SEAM, [pack(ref[0], ref[1], None, None) for ref in (seam_up, seam_mid, seam_down)])
        inner = rows_in & (lane >= 32 - EDGE) & (lane < 32 + EDGE)
        seam_mask = row_mask_of(hub_row, FULL)
        seam = interleave((3 * k, sweep(k, [SEAM], FULL, seam_mask, None, lambda t, lane: inner)) for k in range(ITERS))
        seam_out[...] = xs[ITERS, SEAM, BASE + TOP : BASE + TOP + TR, :] * (1.0 / DSTEP)
        msg[...] = msg[...] + line_of(seam)
        back(2 * Y - 1).start()
        back(2 * Y).start()
        send_sums()

    for here, lanes, cols in (
        (before, lane32 >= 128 - EDGE, slice(TC - 128, TC)), (after, lane32 < EDGE, slice(0, 128))
    ):

        @pl.when(here)
        def _():
            pltpu.make_async_copy(seam_in, seam_in, back_recv).wait()
            out[:, cols] = jnp.where(lanes, pltpu.roll(seam_in[...], 96, 1), out[:, cols])

    def rows_of(ref, n, sem):
        return pltpu.make_async_copy(ref.at[0:n], ref.at[0:n], sem)

    @pl.when(is_root)
    def _():
        part[slot] = msg[...]
        rows_of(part, N_ROW * N_COL - 1, part_recv).wait()
        step = N_ROW * N_COL // 16
        total = [jnp.sum(part[step * i : step * i + step], axis=0) for i in range(16)]
        while len(total) > 1:
            total = [p + q for p, q in zip(total[::2], total[1::2])]
        total = total[0]
        result[...] = total * (1.0 / (CELLS * DSTEP))

        def tell(target):
            pltpu.make_async_remote_copy(
                result, result, result_send, result_recv, device_id=target, device_id_type=pl.DeviceIdType.LOGICAL
            ).start()

        gap[...] = result[...]

        def tell_planes(start, stop):
            @pl.loop(start, stop)
            def _(zz):
                r, c = lax.rem(zz, Z_LO) * X + x, ((zz // Z_LO) * Y + y) * 2
                tell(ident(r, c))
                tell(ident(r, c + 1))

            rows_of(part, 2 * (stop - start), result_send).wait()

        pl.when(hub & (core == 0))(lambda: tell_planes(ALONE + 1, Z))

        @pl.when(hub & (core == 1) & jnp.logical_not(origin))
        def _():
            tell(ident(row, col - 1))
            tell_planes(1, Z)
            rows_of(part, 1, result_send).wait()

        rows_of(part, N_ROOTS - 1, part_send).wait()

    @pl.when(jnp.logical_not(is_root))
    def _():
        pltpu.make_async_copy(result, result, result_recv).wait()
        gap[...] = result[...]
        rows_of(part, N_ROOTS, part_send).wait()

    for dr, dc in SIDES:
        pl.when(exists(dr, dc))(lambda dr=dr, dc=dc: halo(dr, dc).wait_send())
    for side, here in enumerate((before, after)):
        for k in (-1, 0, 1):
            pl.when(here & row_in(row + k))(lambda side=side, k=k: to_hub(side, k).wait_send())

    @pl.when(hub)
    def _():
        back(2 * Y - 1).wait_send()
        back(2 * Y).wait_send()


def finish(denoised, line, out, gap):
    out[...] = denoised[...]
    gap[...] = line[0, :ITERS]


def on_device(noisy):
    f32 = jnp.float32
    vmem = pl.BlockSpec(memory_space=pltpu.VMEM)
    frame = lambda n: pltpu.VMEM((n, NT + 2, BUF, 128), f32)
    dma = pltpu.SemaphoreType.DMA
    denoised, gap = pl.pallas_call(
        kernel,
        out_shape=(jax.ShapeDtypeStruct((TR, TC), f32), jax.ShapeDtypeStruct((1, 128), f32)),
        in_specs=[pl.BlockSpec(memory_space=pltpu.HBM)],
        out_specs=(vmem, vmem),
        scratch_shapes=[
            pltpu.VMEM((TR, TC), f32),
            pltpu.VMEM((8, TC), f32),
            pltpu.VMEM((8, TC), f32),
            pltpu.VMEM((TR, 128), f32),
            pltpu.VMEM((TR, 128), f32),
            pltpu.VMEM((4, 8, 128), f32),
            pltpu.VMEM((2, TR, 128), f32),
            pltpu.VMEM((2, 8, 128), f32),
            pltpu.VMEM((2, 8, 128), f32),
            pltpu.VMEM((TR, 128), f32),
            pltpu.VMEM((TR, 128), f32),
            frame(ITERS + 1), frame(1), frame(ITERS), frame(ITERS), frame(ITERS), frame(ITERS), frame(ITERS), frame(ITERS),
            pltpu.VMEM((1, 128), f32),
            pltpu.VMEM((N_ROW * N_COL, 1, 128), f32),
            pltpu.VMEM((1, 128), f32),
            dma((4,)), dma((8,)), dma((8,)), dma, dma, dma, dma, dma((3,)), dma((6,)), dma((2,)), dma,
        ],
        compiler_params=pltpu.CompilerParams(
            collective_id=0, has_side_effects=True, vmem_limit_bytes=24 * 1024 * 1024
        ),
    )(pltpu.with_memory_space_constraint(noisy, pltpu.HBM))
    return pl.pallas_call(
        finish,
        out_shape=(jax.ShapeDtypeStruct((TR, TC), f32), jax.ShapeDtypeStruct((ITERS,), f32)),
        in_specs=[vmem, vmem],
        out_specs=(vmem, vmem),
        compiler_params=pltpu.CompilerParams(vmem_limit_bytes=4 * 1024 * 1024),
    )(denoised, gap)


def solution(mesh):
    return jax.shard_map(
        on_device,
        mesh=mesh,
        in_specs=(P("row", "col"),),
        out_specs=(P("row", "col"), P()),
        check_vma=False,
    )
```

```python
import jax
import jax.numpy as jnp
from jax import lax
from jax.experimental import pallas as pl
from jax.experimental.pallas import tpu as pltpu
from jax.sharding import PartitionSpec as P

ITERS = 4
Z_LO, X, Z_HI, Y = 8, 4, 2, 4
Z = Z_HI * Z_LO
N_ROW, N_COL = Z_LO * X, Z_HI * Y * 2
ALONE = 2
ROOTS = [(0, 1), (0, 0)] + [(X * i, c) for i in range(1, ALONE + 1) for c in (1, 0)]
ROOTS += [(i // Y, i % Y * 2 + 1) for i in range(1, X * Y)]
N_ROOTS = len(ROOTS)
TR, TC = 32, 2048
NT = TC // 128
FR = 40
BASE = 8
BUF = 56
TOP = 4
STRIP = NT
SEAM = NT + 1
EDGE = 8

FIDELITY = 8.0
PSTEP = 0.35
DSTEP = 0.35
KA = 1.0 / (1.0 + PSTEP * FIDELITY)
KB = PSTEP / (1.0 + PSTEP * FIDELITY)
KC = PSTEP * FIDELITY / (1.0 + PSTEP * FIDELITY)
CELLS = float(N_ROW * TR * N_COL * TC)
TINY = 1e-37
INNER_SKEW = 20
SKEW = 4

SIDES = [(dr, dc) for dr in (-1, 0, 1) for dc in (-1, 0, 1) if (dr, dc) != (0, 0)]


def kernel(
    noisy, out, gap, own, top, bot, lef, rig, corners, seam_mid, seam_up, seam_down, seam_out, seam_in, xs, nc, pr, pc, er, ec, gr, gc,
    msg, part, result, own_sem, send_sem, recv_sem, part_send, part_recv,
    result_send, result_recv, seam_send, seam_recv, back_send, back_recv,
):
    f32 = jnp.float32
    row, col = lax.axis_index("row"), lax.axis_index("col")
    zl, x = row // X, row % X
    zh, y, core = col // (2 * Y), (col // 2) % Y, col % 2
    z = zh * Z_LO + zl

    def lane_of(wins):
        return lax.broadcasted_iota(jnp.int32, (sum(n for _, n in wins), 128), 1)

    def row_of(wins):
        return jnp.concatenate([a + lax.broadcasted_iota(jnp.int32, (n, 128), 0) for a, n in wins], axis=0)

    origin = (x == 0) & (y == 0)
    is_root = ((z == 0) & ((core == 1) | origin)) | ((z >= 1) & (z <= ALONE) & origin)
    before, after = col == 2 * Y - 1, col == 2 * Y
    hub = z == 0
    hub_row = col * X + x

    def ident(r, c):
        return r * N_COL + c

    def hub_of(r):
        return ident(r % X, r // X)

    def exists(dr, dc):
        cond = jnp.logical_not(before if dc > 0 else after) if dc else None
        for t in ([row >= 1] if dr < 0 else [row < N_ROW - 1] if dr > 0 else []) + (
            [col >= 1] if dc < 0 else [col < N_COL - 1] if dc > 0 else []
        ):
            cond = t if cond is None else cond & t
        return cond

    own_copies = [
        pltpu.make_async_copy(noisy.at[8 * i : 8 * i + 8], own.at[8 * i : 8 * i + 8], own_sem.at[i])
        for i in range(TR // 8)
    ]
    for i in (0, 3, 1, 2):
        own_copies[i].start()

    barrier = pltpu.get_barrier_semaphore()

    def signal(target):
        pl.semaphore_signal(barrier, inc=1, device_id=target, device_id_type=pl.DeviceIdType.LOGICAL)

    heard = []
    for dr, dc in SIDES:
        pl.when(exists(dr, dc))(lambda dr=dr, dc=dc: signal(ident(row + dr, col + dc)))
        heard.append(exists(dr, dc))

    def row_in(r):
        return (r >= 0) & (r < N_ROW)

    for k in (-1, 0, 1):
        for c in (2 * Y - 1, 2 * Y):
            pl.when(hub & row_in(hub_row + k))(lambda k=k, c=c: signal(ident(hub_row + k, c)))
        heard.append((before | after) & row_in(row + k))

    @pl.when(is_root)
    def _():
        @pl.loop(0, Z - 1)
        def _(i):
            step = (i + 1) // 2
            zz = (z + jnp.where(i % 2 == 1, Z // 2 - step, Z // 2 + step)) % Z
            for xx in range(X):
                for yc in range(2 * Y):
                    signal(ident((zz % Z_LO) * X + xx, (zz // Z_LO) * 2 * Y + yc))

        for xx in range(X):
            for yc in range(2 * Y):
                pl.when((x != xx) | (y * 2 + core != yc))(lambda xx=xx, yc=yc: signal(ident(zl * X + xx, zh * 2 * Y + yc)))

    gone = (
        (row == 0, top), (row == N_ROW - 1, bot), ((col == 0) | after, lef), ((col == N_COL - 1) | before, rig),
        (hub & (hub_row == 0), seam_up), (hub & (hub_row == N_ROW - 1), seam_down),
    )
    for cond, buf in gone:

        @pl.when(cond)
        def _():
            buf[...] = jnp.zeros_like(buf)

    for i, (dr, dc) in enumerate([(-1, -1), (-1, 1), (1, -1), (1, 1)]):

        @pl.when(jnp.logical_not(exists(dr, dc)))
        def _():
            corners[i] = jnp.zeros((8, 128), f32)

    for k in range(ITERS):
        for t in range(NT + 2):
            pr[k, t, 0:BASE, :] = jnp.zeros((BASE, 128), f32)

    own_copies[0].wait()
    own_copies[3].wait()
    count = jnp.where(is_root, N_ROOTS - 1, N_ROOTS)
    for hear in heard:
        count = count + jnp.where(hear, 1, 0)
    pl.semaphore_wait(barrier, count)

    place0 = {
        (-1, 0): top, (1, 0): bot, (0, -1): lef, (0, 1): rig, (-1, -1): corners.at[0], (-1, 1): corners.at[1],
        (1, -1): corners.at[2], (1, 1): corners.at[3],
    }

    place = {k: (v if k[0] == 0 else v.at[4:8] if k[0] < 0 else v.at[0:5]) for k, v in place0.items()}

    def source(dr, dc):
        rs = slice(0, TR) if dr == 0 else slice(0, 5) if dr < 0 else slice(TR - 4, TR)
        cs = slice(0, TC) if dc == 0 else slice(0, 128) if dc < 0 else slice(TC - 128, TC)
        return own.at[rs, cs]

    def halo(dr, dc):
        i = SIDES.index((dr, dc))
        return pltpu.make_async_remote_copy(
            source(dr, dc), place[(-dr, -dc)], send_sem.at[i], recv_sem.at[SIDES.index((-dr, -dc))],
            device_id=ident(row + dr, col + dc), device_id_type=pl.DeviceIdType.LOGICAL,
        )

    def arrived(dr, dc):
        i = SIDES.index((dr, dc))
        return pltpu.make_async_remote_copy(
            source(-dr, -dc), place[(dr, dc)], send_sem.at[i], recv_sem.at[i],
            device_id=ident(row, col), device_id_type=pl.DeviceIdType.LOGICAL,
        )

    for dr, dc in [(1, 1), (1, -1), (-1, 1), (-1, -1), (1, 0), (-1, 0), (0, 1), (0, -1)]:
        if (dr, dc) == (0, 1):
            own_copies[1].wait()
            own_copies[2].wait()
        pl.when(exists(dr, dc))(lambda dr=dr, dc=dc: halo(dr, dc).start())

    def to_hub(side, k):
        ref = (seam_down, seam_mid, seam_up)[k + 1]
        rs = (slice(0, 8), slice(0, TR), slice(TR - 8, TR))[k + 1]
        cs = (slice(TC - 128, TC), slice(0, 128))[side]
        i = side * 3 + k + 1
        return pltpu.make_async_remote_copy(
            own.at[rs, cs], ref.at[side], seam_send.at[k + 1], seam_recv.at[i],
            device_id=hub_of(row + k), device_id_type=pl.DeviceIdType.LOGICAL,
        )

    for side, here in enumerate((before, after)):
        for k in (0, -1, 1):
            pl.when(here & row_in(row + k))(lambda side=side, k=k: to_hub(side, k).start())

    def row_mask_of(r, wins):
        grow = r * TR - TOP + row_of(wins)
        return jnp.where((grow >= 0) & (grow < N_ROW * TR - 1), 1.0, 0.0).astype(f32)

    def load(ref, k, t, wins, shift=0):
        return jnp.concatenate([ref[k, t, BASE + a + shift : BASE + a + shift + n, :] for a, n in wins], axis=0)

    def store(ref, k, t, wins, v):
        at = 0
        for a, n in wins:
            ref[k, t, BASE + a : BASE + a + n, :] = v[at : at + n]
            at += n

    def left_of(v):
        return pltpu.roll(v, 1, 1)

    def right_of(v):
        return pltpu.roll(v, 127, 1)

    def sums(cell):
        acc = cell[0:8]
        for i in range(1, cell.shape[0] // 8):
            acc = acc + cell[8 * i : 8 * i + 8]
        return acc

    def sweep(k, tiles, wins, row_mask, col_mask, keep):
        def masked(v, mask):
            return v if mask is None else v * mask

        total = prev_pc = pend = rolled_n = None
        lane = lane_of(wins)
        for t in tiles + [None]:
            if t is not None:
                n = load(xs, 0, t, wins)
                if k == 0:
                    ncol = right_of(n) if rolled_n is None else rolled_n
                    nright = ncol
                    if t != tiles[-1]:
                        rolled_n = right_of(load(xs, 0, t + 1, wins))
                        nright = jnp.where(lane == 127, rolled_n, ncol)
                    qr = masked(load(xs, 0, t, wins, 1) - n, row_mask)
                    qc = masked(nright - n, col_mask)
                    store(gr, 0, t, wins, qr)
                    store(gc, 0, t, wins, qc)
                else:
                    qr = load(pr, k - 1, t, wins) + load(er, k - 1, t, wins)
                    qc = load(pc, k - 1, t, wins) + load(ec, k - 1, t, wins)
                shrink = lax.rsqrt(jnp.maximum(qr * qr + qc * qc, 1.0))
                p_r = qr * shrink
                p_c = qc * shrink
                store(pr, k, t, wins, p_r)
                if k < ITERS - 1:
                    store(pc, k, t, wins, p_c)
                rolled = left_of(p_c)
                pleft = rolled if prev_pc is None else jnp.where(lane == 0, prev_pc, rolled)
                prev_pc = rolled
                d = (p_r - load(pr, k, t, wins, -1)) + (p_c - pleft)
                if k == 0:
                    new = n + (KB * DSTEP) * d
                    store(nc, 0, t, wins, n * KC)
                else:
                    new = KA * load(xs, k, t, wins) + ((KB * DSTEP) * d + load(nc, 0, t, wins))
                store(xs, k + 1, t, wins, new)
                rolled_x = right_of(new)
            if pend is not None:
                s, sx, sd, sn, srolled = pend
                xright = srolled if t is None else jnp.where(lane == 127, rolled_x, srolled)
                g_r = masked(load(xs, k + 1, s, wins, 1) - sx, row_mask)
                g_c = masked(xright - sx, col_mask)
                if k < ITERS - 1:
                    store(er, k, s, wins, g_r + (g_r - load(gr, k, s, wins)))
                    store(ec, k, s, wins, g_c + (g_c - load(gc, k, s, wins)))
                if k < ITERS - 2:
                    store(gr, k + 1, s, wins, g_r)
                    store(gc, k + 1, s, wins, g_c)
                m = g_r * g_r + g_c * g_c
                size = m * lax.rsqrt(jnp.maximum(m, TINY))
                diff = sx - sn
                cell = (diff * diff) * (0.5 * FIDELITY / DSTEP) + sd * (sn + sd * (0.5 * DSTEP / FIDELITY))
                cell = sums(jnp.where(keep(s, lane), cell + size, 0.0))
                total = cell if total is None else total + cell
            if t is not None:
                pend = (t, new, d, n, rolled_x)
            yield
        return total

    def interleave(work):
        work = [list(w) for w in work]
        results = [None] * len(work)
        step = 0
        while any(g is not None for _, g in work):
            for i, (start, g) in enumerate(work):
                if g is not None and step >= start:
                    try:
                        next(g)
                    except StopIteration as end:
                        results[i] = end.value
                        work[i][1] = None
            step += 1
        return results

    def wait_side(dr, dc):
        pl.when(exists(dr, dc))(lambda: arrived(dr, dc).wait_recv())

    def columns(t, lane):
        if t == 0:
            return lane >= EDGE
        if t == NT - 1:
            return lane < 128 - EDGE
        return None

    def keep_rows(wins, first, last):
        a = row_of(wins)
        inside = (a >= TOP + first) & (a <= TOP + last)

        def keep(t, lane):
            here = columns(t, lane)
            return inside if here is None else inside & here

        return keep

    MAIN = list(range(NT))
    FULL = [(0, FR)]
    INNER = [(TOP, TR)]
    for t in MAIN:
        xs[0, t, BASE + TOP : BASE + TOP + TR, :] = own[:, 128 * t : 128 * t + 128] * DSTEP
    acc = interleave(
        (k * INNER_SKEW, sweep(k, MAIN, INNER, None, None, keep_rows(INNER, k + 1, TR - 3 - k)))
        for k in range(ITERS)
    )

    wait_side(-1, 0)
    wait_side(1, 0)
    for dr in (-1, 0, 1):
        wait_side(dr, -1)
        wait_side(dr, 1)
    for t in MAIN:
        cs = slice(128 * t, 128 * t + 128)
        xs[0, t, BASE + TOP - 8 : BASE + TOP, :] = top[:, cs] * DSTEP
        xs[0, t, BASE + TOP + TR : BASE + TOP + TR + 8, :] = bot[:, cs] * DSTEP

    def pack(last, right, left, first):
        q = lax.broadcasted_iota(jnp.int32, last.shape, 1)
        v = jnp.where(q < 32, pltpu.roll(last, 32, 1), pltpu.roll(right, 32, 1))
        if left is None:
            return v
        w = jnp.where(q < 96, pltpu.roll(left, 96, 1), pltpu.roll(first, 96, 1))
        return jnp.where(q < 64, v, w)

    def fill(t, parts):
        xs[0, t, BASE + TOP - 8 : BASE + TOP, :] = parts[0] * DSTEP
        xs[0, t, BASE + TOP : BASE + TOP + TR, :] = parts[1] * DSTEP
        xs[0, t, BASE + TOP + TR : BASE + TOP + TR + 8, :] = parts[2] * DSTEP

    lo, hi = slice(0, 128), slice(TC - 128, TC)
    fill(STRIP, [
        pack(top[:, hi], corners[1], corners[0], top[:, lo]),
        pack(own[:, hi], rig[...], lef[...], own[:, lo]),
        pack(bot[:, hi], corners[3], corners[2], bot[:, lo]),
    ])
    lane = lane_of(FULL)
    outside = ((col == 0) & (lane >= 64) & (lane < 96)) | ((col == N_COL - 1) & (lane >= 31) & (lane < 64))
    strip_mask = jnp.where(outside, 0.0, 1.0).astype(f32)
    rows_in = (row_of(FULL) >= TOP) & (row_of(FULL) < TOP + TR)
    owned = jnp.logical_not(before) & (lane >= 32 - EDGE) & (lane < 32)
    owned = owned | (jnp.logical_not(after) & (lane >= 96) & (lane < 96 + EDGE))
    owned = owned & rows_in
    full_mask = row_mask_of(row, FULL)
    work = []
    for k in range(ITERS):
        wins = [(k, 8), (32 - k, 8)]
        rows = row_of(wins)
        edge = ((rows >= TOP) & (rows <= TOP + k)) | ((rows >= TOP + TR - 2 - k) & (rows < TOP + TR))

        def keep(t, lane, edge=edge):
            here = columns(t, lane)
            return edge if here is None else edge & here

        work.append((k * SKEW, sweep(k, MAIN, wins, row_mask_of(row, wins), None, keep)))
        work.append((k * SKEW, sweep(k, [STRIP], FULL, full_mask, strip_mask, lambda t, lane: owned)))
    done = interleave(work)
    acc = [acc[k] + done[2 * k] + done[2 * k + 1] for k in range(ITERS)]

    lane8 = lax.broadcasted_iota(jnp.int32, (8, 128), 1)

    def line_of(acc):
        table = jnp.zeros((8, 128), f32)
        for k in range(ITERS):
            table = jnp.where(lane8 == k, jnp.sum(acc[k], axis=1, keepdims=True), table)
        return jnp.sum(table, axis=0, keepdims=True)

    msg[...] = line_of(acc)

    slot = ident(row, col)

    def send_sums():
        for xx, yc in ROOTS:

            @pl.when((row != xx) | (col != yc))
            def _():
                pltpu.make_async_remote_copy(
                    msg, part.at[pl.ds(slot, 1)], part_send, part_recv,
                    device_id=ident(xx, yc), device_id_type=pl.DeviceIdType.LOGICAL,
                ).start()

    pl.when(jnp.logical_not(hub))(send_sums)

    lane32 = lax.broadcasted_iota(jnp.int32, (TR, 128), 1)
    for t in range(NT):
        v = xs[ITERS, t, BASE + TOP : BASE + TOP + TR, :]
        if t in (0, NT - 1):
            s = xs[ITERS, STRIP, BASE + TOP : BASE + TOP + TR, :]
            if t == 0:
                v = jnp.where(lane32 < EDGE, pltpu.roll(s, 32, 1), v)
            else:
                v = jnp.where(lane32 >= 128 - EDGE, pltpu.roll(s, 96, 1), v)
        out[:, 128 * t : 128 * t + 128] = v * (1.0 / DSTEP)

    def back(c):
        return pltpu.make_async_remote_copy(
            seam_out, seam_in, back_send.at[c - (2 * Y - 1)], back_recv,
            device_id=ident(hub_row, c), device_id_type=pl.DeviceIdType.LOGICAL,
        )

    @pl.when(hub)
    def _():
        for side in (0, 1):
            for k in (-1, 0, 1):
                ref = (seam_up, seam_mid, seam_down)[k + 1]
                i = side * 3 - k + 1

                @pl.when(row_in(hub_row + k))
                def _():
                    pltpu.make_async_copy(ref.at[side], ref.at[side], seam_recv.at[i]).wait()

        fill(SEAM, [pack(ref[0], ref[1], None, None) for ref in (seam_up, seam_mid, seam_down)])
        inner = rows_in & (lane >= 32 - EDGE) & (lane < 32 + EDGE)
        seam_mask = row_mask_of(hub_row, FULL)
        seam = interleave((3 * k, sweep(k, [SEAM], FULL, seam_mask, None, lambda t, lane: inner)) for k in range(ITERS))
        seam_out[...] = xs[ITERS, SEAM, BASE + TOP : BASE + TOP + TR, :] * (1.0 / DSTEP)
        msg[...] = msg[...] + line_of(seam)
        back(2 * Y - 1).start()
        back(2 * Y).start()
        send_sums()

    for here, lanes, cols in (
        (before, lane32 >= 128 - EDGE, slice(TC - 128, TC)), (after, lane32 < EDGE, slice(0, 128))
    ):

        @pl.when(here)
        def _():
            pltpu.make_async_copy(seam_in, seam_in, back_recv).wait()
            out[:, cols] = jnp.where(lanes, pltpu.roll(seam_in[...], 96, 1), out[:, cols])

    def rows_of(ref, n, sem):
        return pltpu.make_async_copy(ref.at[0:n], ref.at[0:n], sem)

    for dr, dc in SIDES:
        pl.when(exists(dr, dc))(lambda dr=dr, dc=dc: halo(dr, dc).wait_send())
    for side, here in enumerate((before, after)):
        for k in (-1, 0, 1):
            pl.when(here & row_in(row + k))(lambda side=side, k=k: to_hub(side, k).wait_send())

    @pl.when(hub)
    def _():
        back(2 * Y - 1).wait_send()
        back(2 * Y).wait_send()

    pl.when(is_root)(lambda: rows_of(part, N_ROOTS - 1, part_send).wait())
    pl.when(jnp.logical_not(is_root))(lambda: rows_of(part, N_ROOTS, part_send).wait())

    @pl.when(is_root)
    def _():
        part[pl.ds(slot, 1), :] = msg[...]
        rows_of(part, N_ROW * N_COL - 1, part_recv).wait()
        total = [part[8 * i : 8 * i + 8] for i in range(N_ROW * N_COL // 8)]
        while len(total) > 1:
            total = [p + q for p, q in zip(total[::2], total[1::2])]
        total = jnp.sum(total[0], axis=0, keepdims=True)
        result[...] = total * (1.0 / (CELLS * DSTEP))

        def tell(target):
            pltpu.make_async_remote_copy(
                result, result, result_send, result_recv, device_id=target, device_id_type=pl.DeviceIdType.LOGICAL
            ).start()

        gap[...] = result[...]

        def tell_planes(start, stop):
            @pl.loop(start, stop)
            def _(zz):
                r, c = lax.rem(zz, Z_LO) * X + x, ((zz // Z_LO) * Y + y) * 2
                tell(ident(r, c))
                tell(ident(r, c + 1))

            rows_of(part, 2 * (stop - start), result_send).wait()

        pl.when(hub & (core == 0))(lambda: tell_planes(ALONE + 1, Z))

        @pl.when(hub & (core == 1) & jnp.logical_not(origin))
        def _():
            tell(ident(row, col - 1))
            tell_planes(1, Z)
            rows_of(part, 1, result_send).wait()


    @pl.when(jnp.logical_not(is_root))
    def _():
        pltpu.make_async_copy(result, result, result_recv).wait()
        gap[...] = result[...]


def finish(denoised, line, out, gap):
    out[...] = denoised[...]
    gap[...] = line[0, :ITERS]


def on_device(noisy):
    f32 = jnp.float32
    vmem = pl.BlockSpec(memory_space=pltpu.VMEM)
    frame = lambda n: pltpu.VMEM((n, NT + 2, BUF, 128), f32)
    dma = pltpu.SemaphoreType.DMA
    denoised, gap = pl.pallas_call(
        kernel,
        out_shape=(jax.ShapeDtypeStruct((TR, TC), f32), jax.ShapeDtypeStruct((1, 128), f32)),
        in_specs=[pl.BlockSpec(memory_space=pltpu.HBM)],
        out_specs=(vmem, vmem),
        scratch_shapes=[
            pltpu.VMEM((TR, TC), f32),
            pltpu.VMEM((8, TC), f32),
            pltpu.VMEM((8, TC), f32),
            pltpu.VMEM((TR, 128), f32),
            pltpu.VMEM((TR, 128), f32),
            pltpu.VMEM((4, 8, 128), f32),
            pltpu.VMEM((2, TR, 128), f32),
            pltpu.VMEM((2, 8, 128), f32),
            pltpu.VMEM((2, 8, 128), f32),
            pltpu.VMEM((TR, 128), f32),
            pltpu.VMEM((TR, 128), f32),
            frame(ITERS + 1), frame(1), frame(ITERS), frame(ITERS), frame(ITERS), frame(ITERS), frame(ITERS), frame(ITERS),
            pltpu.VMEM((1, 128), f32),
            pltpu.VMEM((N_ROW * N_COL, 128), f32),
            pltpu.VMEM((1, 128), f32),
            dma((4,)), dma((8,)), dma((8,)), dma, dma, dma, dma, dma((3,)), dma((6,)), dma((2,)), dma,
        ],
        compiler_params=pltpu.CompilerParams(
            collective_id=0, has_side_effects=True, vmem_limit_bytes=24 * 1024 * 1024
        ),
    )(pltpu.with_memory_space_constraint(noisy, pltpu.HBM))
    return pl.pallas_call(
        finish,
        out_shape=(jax.ShapeDtypeStruct((TR, TC), f32), jax.ShapeDtypeStruct((ITERS,), f32)),
        in_specs=[vmem, vmem],
        out_specs=(vmem, vmem),
        compiler_params=pltpu.CompilerParams(vmem_limit_bytes=4 * 1024 * 1024),
    )(denoised, gap)


def solution(mesh):
    return jax.shard_map(
        on_device,
        mesh=mesh,
        in_specs=(P("row", "col"),),
        out_specs=(P("row", "col"), P()),
        check_vma=False,
    )
```

```python
import jax
import jax.numpy as jnp
from jax import lax
from jax.experimental import pallas as pl
from jax.experimental.pallas import tpu as pltpu
from jax.sharding import PartitionSpec as P

ITERS = 4
Z_LO, X, Z_HI, Y = 8, 4, 2, 4
Z = Z_HI * Z_LO
N_ROW, N_COL = Z_LO * X, Z_HI * Y * 2
ALONE = 3
ROOTS = [(0, 1), (0, 0)] + [(X * i, c) for i in range(1, ALONE + 1) for c in (1, 0)]
ROOTS += [(i // Y, i % Y * 2 + 1) for i in range(1, X * Y)]
N_ROOTS = len(ROOTS)
TR, TC = 32, 2048
NT = TC // 128
FR = 40
BASE = 8
BUF = 56
TOP = 4
STRIP = NT
SEAM = NT + 1
EDGE = 8

FIDELITY = 8.0
PSTEP = 0.35
DSTEP = 0.35
KA = 1.0 / (1.0 + PSTEP * FIDELITY)
KB = PSTEP / (1.0 + PSTEP * FIDELITY)
KC = PSTEP * FIDELITY / (1.0 + PSTEP * FIDELITY)
CELLS = float(N_ROW * TR * N_COL * TC)
TINY = 1e-37
INNER_SKEW = 20
SKEW = 4

SIDES = [(dr, dc) for dr in (-1, 0, 1) for dc in (-1, 0, 1) if (dr, dc) != (0, 0)]


def kernel(
    noisy, out, gap, own, top, bot, lef, rig, corners, seam_mid, seam_up, seam_down, seam_out, seam_in, xs, nc, pr, pc, er, ec, gr, gc,
    msg, part, result, own_sem, send_sem, recv_sem, part_send, part_recv,
    result_send, result_recv, seam_send, seam_recv, back_send, back_recv,
):
    f32 = jnp.float32
    row, col = lax.axis_index("row"), lax.axis_index("col")
    zl, x = row // X, row % X
    zh, y, core = col // (2 * Y), (col // 2) % Y, col % 2
    z = zh * Z_LO + zl

    def lane_of(wins):
        return lax.broadcasted_iota(jnp.int32, (sum(n for _, n in wins), 128), 1)

    def row_of(wins):
        return jnp.concatenate([a + lax.broadcasted_iota(jnp.int32, (n, 128), 0) for a, n in wins], axis=0)

    origin = (x == 0) & (y == 0)
    is_root = ((z == 0) & ((core == 1) | origin)) | ((z >= 1) & (z <= ALONE) & origin)
    before, after = col == 2 * Y - 1, col == 2 * Y
    hub = z == 0
    hub_row = col * X + x

    def ident(r, c):
        return r * N_COL + c

    def hub_of(r):
        return ident(r % X, r // X)

    def exists(dr, dc):
        cond = jnp.logical_not(before if dc > 0 else after) if dc else None
        for t in ([row >= 1] if dr < 0 else [row < N_ROW - 1] if dr > 0 else []) + (
            [col >= 1] if dc < 0 else [col < N_COL - 1] if dc > 0 else []
        ):
            cond = t if cond is None else cond & t
        return cond

    own_copies = [
        pltpu.make_async_copy(noisy.at[8 * i : 8 * i + 8], own.at[8 * i : 8 * i + 8], own_sem.at[i])
        for i in range(TR // 8)
    ]
    for i in (0, 3, 1, 2):
        own_copies[i].start()

    barrier = pltpu.get_barrier_semaphore()

    def signal(target):
        pl.semaphore_signal(barrier, inc=1, device_id=target, device_id_type=pl.DeviceIdType.LOGICAL)

    heard = []
    for dr, dc in SIDES:
        pl.when(exists(dr, dc))(lambda dr=dr, dc=dc: signal(ident(row + dr, col + dc)))
        heard.append(exists(dr, dc))

    def row_in(r):
        return (r >= 0) & (r < N_ROW)

    for k in (-1, 0, 1):
        for c in (2 * Y - 1, 2 * Y):
            pl.when(hub & row_in(hub_row + k))(lambda k=k, c=c: signal(ident(hub_row + k, c)))
        heard.append((before | after) & row_in(row + k))

    @pl.when(is_root)
    def _():
        @pl.loop(0, Z - 1)
        def _(i):
            step = (i + 1) // 2
            zz = (z + jnp.where(i % 2 == 1, Z // 2 - step, Z // 2 + step)) % Z
            for xx in range(X):
                for yc in range(2 * Y):
                    signal(ident((zz % Z_LO) * X + xx, (zz // Z_LO) * 2 * Y + yc))

        for xx in range(X):
            for yc in range(2 * Y):
                pl.when((x != xx) | (y * 2 + core != yc))(lambda xx=xx, yc=yc: signal(ident(zl * X + xx, zh * 2 * Y + yc)))

    gone = (
        (row == 0, top), (row == N_ROW - 1, bot), ((col == 0) | after, lef), ((col == N_COL - 1) | before, rig),
        (hub & (hub_row == 0), seam_up), (hub & (hub_row == N_ROW - 1), seam_down),
    )
    for cond, buf in gone:

        @pl.when(cond)
        def _():
            buf[...] = jnp.zeros_like(buf)

    for i, (dr, dc) in enumerate([(-1, -1), (-1, 1), (1, -1), (1, 1)]):

        @pl.when(jnp.logical_not(exists(dr, dc)))
        def _():
            corners[i] = jnp.zeros((8, 128), f32)

    for k in range(ITERS):
        for t in range(NT + 2):
            pr[k, t, 0:BASE, :] = jnp.zeros((BASE, 128), f32)

    own_copies[0].wait()
    own_copies[3].wait()
    count = jnp.where(is_root, N_ROOTS - 1, N_ROOTS)
    for hear in heard:
        count = count + jnp.where(hear, 1, 0)
    pl.semaphore_wait(barrier, count)

    place0 = {
        (-1, 0): top, (1, 0): bot, (0, -1): lef, (0, 1): rig, (-1, -1): corners.at[0], (-1, 1): corners.at[1],
        (1, -1): corners.at[2], (1, 1): corners.at[3],
    }

    place = {k: (v if k[0] == 0 else v.at[4:8] if k[0] < 0 else v.at[0:5]) for k, v in place0.items()}

    def source(dr, dc):
        rs = slice(0, TR) if dr == 0 else slice(0, 5) if dr < 0 else slice(TR - 4, TR)
        cs = slice(0, TC) if dc == 0 else slice(0, 128) if dc < 0 else slice(TC - 128, TC)
        return own.at[rs, cs]

    def halo(dr, dc):
        i = SIDES.index((dr, dc))
        return pltpu.make_async_remote_copy(
            source(dr, dc), place[(-dr, -dc)], send_sem.at[i], recv_sem.at[SIDES.index((-dr, -dc))],
            device_id=ident(row + dr, col + dc), device_id_type=pl.DeviceIdType.LOGICAL,
        )

    def arrived(dr, dc):
        i = SIDES.index((dr, dc))
        return pltpu.make_async_remote_copy(
            source(-dr, -dc), place[(dr, dc)], send_sem.at[i], recv_sem.at[i],
            device_id=ident(row, col), device_id_type=pl.DeviceIdType.LOGICAL,
        )

    for dr, dc in [(1, 1), (1, -1), (-1, 1), (-1, -1), (1, 0), (-1, 0), (0, 1), (0, -1)]:
        if (dr, dc) == (0, 1):
            own_copies[1].wait()
            own_copies[2].wait()
        pl.when(exists(dr, dc))(lambda dr=dr, dc=dc: halo(dr, dc).start())

    def to_hub(side, k):
        ref = (seam_down, seam_mid, seam_up)[k + 1]
        rs = (slice(0, 8), slice(0, TR), slice(TR - 8, TR))[k + 1]
        cs = (slice(TC - 128, TC), slice(0, 128))[side]
        i = side * 3 + k + 1
        return pltpu.make_async_remote_copy(
            own.at[rs, cs], ref.at[side], seam_send.at[k + 1], seam_recv.at[i],
            device_id=hub_of(row + k), device_id_type=pl.DeviceIdType.LOGICAL,
        )

    for side, here in enumerate((before, after)):
        for k in (0, -1, 1):
            pl.when(here & row_in(row + k))(lambda side=side, k=k: to_hub(side, k).start())

    def row_mask_of(r, wins):
        grow = r * TR - TOP + row_of(wins)
        return jnp.where((grow >= 0) & (grow < N_ROW * TR - 1), 1.0, 0.0).astype(f32)

    def load(ref, k, t, wins, shift=0):
        return jnp.concatenate([ref[k, t, BASE + a + shift : BASE + a + shift + n, :] for a, n in wins], axis=0)

    def store(ref, k, t, wins, v):
        at = 0
        for a, n in wins:
            ref[k, t, BASE + a : BASE + a + n, :] = v[at : at + n]
            at += n

    def left_of(v):
        return pltpu.roll(v, 1, 1)

    def right_of(v):
        return pltpu.roll(v, 127, 1)

    def sums(cell):
        acc = cell[0:8]
        for i in range(1, cell.shape[0] // 8):
            acc = acc + cell[8 * i : 8 * i + 8]
        return acc

    def sweep(k, tiles, wins, row_mask, col_mask, keep):
        def masked(v, mask):
            return v if mask is None else v * mask

        total = prev_pc = pend = rolled_n = None
        lane = lane_of(wins)
        for t in tiles + [None]:
            if t is not None:
                n = load(xs, 0, t, wins)
                if k == 0:
                    ncol = right_of(n) if rolled_n is None else rolled_n
                    nright = ncol
                    if t != tiles[-1]:
                        rolled_n = right_of(load(xs, 0, t + 1, wins))
                        nright = jnp.where(lane == 127, rolled_n, ncol)
                    qr = masked(load(xs, 0, t, wins, 1) - n, row_mask)
                    qc = masked(nright - n, col_mask)
                    store(gr, 0, t, wins, qr)
                    store(gc, 0, t, wins, qc)
                else:
                    qr = load(pr, k - 1, t, wins) + load(er, k - 1, t, wins)
                    qc = load(pc, k - 1, t, wins) + load(ec, k - 1, t, wins)
                shrink = lax.rsqrt(jnp.maximum(qr * qr + qc * qc, 1.0))
                p_r = qr * shrink
                p_c = qc * shrink
                store(pr, k, t, wins, p_r)
                if k < ITERS - 1:
                    store(pc, k, t, wins, p_c)
                rolled = left_of(p_c)
                pleft = rolled if prev_pc is None else jnp.where(lane == 0, prev_pc, rolled)
                prev_pc = rolled
                d = (p_r - load(pr, k, t, wins, -1)) + (p_c - pleft)
                if k == 0:
                    new = n + (KB * DSTEP) * d
                    store(nc, 0, t, wins, n * KC)
                else:
                    new = KA * load(xs, k, t, wins) + ((KB * DSTEP) * d + load(nc, 0, t, wins))
                store(xs, k + 1, t, wins, new)
                rolled_x = right_of(new)
            if pend is not None:
                s, sx, sd, sn, srolled = pend
                xright = srolled if t is None else jnp.where(lane == 127, rolled_x, srolled)
                g_r = masked(load(xs, k + 1, s, wins, 1) - sx, row_mask)
                g_c = masked(xright - sx, col_mask)
                if k < ITERS - 1:
                    store(er, k, s, wins, g_r + (g_r - load(gr, k, s, wins)))
                    store(ec, k, s, wins, g_c + (g_c - load(gc, k, s, wins)))
                if k < ITERS - 2:
                    store(gr, k + 1, s, wins, g_r)
                    store(gc, k + 1, s, wins, g_c)
                m = g_r * g_r + g_c * g_c
                size = m * lax.rsqrt(jnp.maximum(m, TINY))
                diff = sx - sn
                cell = (diff * diff) * (0.5 * FIDELITY / DSTEP) + sd * (sn + sd * (0.5 * DSTEP / FIDELITY))
                cell = sums(jnp.where(keep(s, lane), cell + size, 0.0))
                total = cell if total is None else total + cell
            if t is not None:
                pend = (t, new, d, n, rolled_x)
            yield
        return total

    def interleave(work):
        work = [list(w) for w in work]
        results = [None] * len(work)
        step = 0
        while any(g is not None for _, g in work):
            for i, (start, g) in enumerate(work):
                if g is not None and step >= start:
                    try:
                        next(g)
                    except StopIteration as end:
                        results[i] = end.value
                        work[i][1] = None
            step += 1
        return results

    def wait_side(dr, dc):
        pl.when(exists(dr, dc))(lambda: arrived(dr, dc).wait_recv())

    def columns(t, lane):
        if t == 0:
            return lane >= EDGE
        if t == NT - 1:
            return lane < 128 - EDGE
        return None

    def keep_rows(wins, first, last):
        a = row_of(wins)
        inside = (a >= TOP + first) & (a <= TOP + last)

        def keep(t, lane):
            here = columns(t, lane)
            return inside if here is None else inside & here

        return keep

    MAIN = list(range(NT))
    FULL = [(0, FR)]
    INNER = [(TOP, TR)]
    for t in MAIN:
        xs[0, t, BASE + TOP : BASE + TOP + TR, :] = own[:, 128 * t : 128 * t + 128] * DSTEP
    acc = interleave(
        (k * INNER_SKEW, sweep(k, MAIN, INNER, None, None, keep_rows(INNER, k + 1, TR - 3 - k)))
        for k in range(ITERS)
    )

    wait_side(-1, 0)
    wait_side(1, 0)
    for dr in (-1, 0, 1):
        wait_side(dr, -1)
        wait_side(dr, 1)
    for t in MAIN:
        cs = slice(128 * t, 128 * t + 128)
        xs[0, t, BASE + TOP - 8 : BASE + TOP, :] = top[:, cs] * DSTEP
        xs[0, t, BASE + TOP + TR : BASE + TOP + TR + 8, :] = bot[:, cs] * DSTEP

    def pack(last, right, left, first):
        q = lax.broadcasted_iota(jnp.int32, last.shape, 1)
        v = jnp.where(q < 32, pltpu.roll(last, 32, 1), pltpu.roll(right, 32, 1))
        if left is None:
            return v
        w = jnp.where(q < 96, pltpu.roll(left, 96, 1), pltpu.roll(first, 96, 1))
        return jnp.where(q < 64, v, w)

    def fill(t, parts):
        xs[0, t, BASE + TOP - 8 : BASE + TOP, :] = parts[0] * DSTEP
        xs[0, t, BASE + TOP : BASE + TOP + TR, :] = parts[1] * DSTEP
        xs[0, t, BASE + TOP + TR : BASE + TOP + TR + 8, :] = parts[2] * DSTEP

    lo, hi = slice(0, 128), slice(TC - 128, TC)
    fill(STRIP, [
        pack(top[:, hi], corners[1], corners[0], top[:, lo]),
        pack(own[:, hi], rig[...], lef[...], own[:, lo]),
        pack(bot[:, hi], corners[3], corners[2], bot[:, lo]),
    ])
    lane = lane_of(FULL)
    outside = ((col == 0) & (lane >= 64) & (lane < 96)) | ((col == N_COL - 1) & (lane >= 31) & (lane < 64))
    strip_mask = jnp.where(outside, 0.0, 1.0).astype(f32)
    rows_in = (row_of(FULL) >= TOP) & (row_of(FULL) < TOP + TR)
    owned = jnp.logical_not(before) & (lane >= 32 - EDGE) & (lane < 32)
    owned = owned | (jnp.logical_not(after) & (lane >= 96) & (lane < 96 + EDGE))
    owned = owned & rows_in
    full_mask = row_mask_of(row, FULL)
    work = []
    for k in range(ITERS):
        wins = [(k, 8), (32 - k, 8)]
        rows = row_of(wins)
        edge = ((rows >= TOP) & (rows <= TOP + k)) | ((rows >= TOP + TR - 2 - k) & (rows < TOP + TR))

        def keep(t, lane, edge=edge):
            here = columns(t, lane)
            return edge if here is None else edge & here

        work.append((k * SKEW, sweep(k, MAIN, wins, row_mask_of(row, wins), None, keep)))
        work.append((k * SKEW, sweep(k, [STRIP], FULL, full_mask, strip_mask, lambda t, lane: owned)))
    done = interleave(work)
    acc = [acc[k] + done[2 * k] + done[2 * k + 1] for k in range(ITERS)]

    lane8 = lax.broadcasted_iota(jnp.int32, (8, 128), 1)

    def line_of(acc):
        table = jnp.zeros((8, 128), f32)
        for k in range(ITERS):
            table = jnp.where(lane8 == k, jnp.sum(acc[k], axis=1, keepdims=True), table)
        return jnp.sum(table, axis=0, keepdims=True)

    msg[...] = line_of(acc)

    slot = ident(row, col)

    def send_sums():
        for xx, yc in ROOTS:

            @pl.when((row != xx) | (col != yc))
            def _():
                pltpu.make_async_remote_copy(
                    msg, part.at[pl.ds(slot, 1)], part_send, part_recv,
                    device_id=ident(xx, yc), device_id_type=pl.DeviceIdType.LOGICAL,
                ).start()

    pl.when(jnp.logical_not(hub))(send_sums)

    lane32 = lax.broadcasted_iota(jnp.int32, (TR, 128), 1)
    for t in range(NT):
        v = xs[ITERS, t, BASE + TOP : BASE + TOP + TR, :]
        if t in (0, NT - 1):
            s = xs[ITERS, STRIP, BASE + TOP : BASE + TOP + TR, :]
            if t == 0:
                v = jnp.where(lane32 < EDGE, pltpu.roll(s, 32, 1), v)
            else:
                v = jnp.where(lane32 >= 128 - EDGE, pltpu.roll(s, 96, 1), v)
        out[:, 128 * t : 128 * t + 128] = v * (1.0 / DSTEP)

    def back(c):
        return pltpu.make_async_remote_copy(
            seam_out, seam_in, back_send.at[c - (2 * Y - 1)], back_recv,
            device_id=ident(hub_row, c), device_id_type=pl.DeviceIdType.LOGICAL,
        )

    @pl.when(hub)
    def _():
        for side in (0, 1):
            for k in (-1, 0, 1):
                ref = (seam_up, seam_mid, seam_down)[k + 1]
                i = side * 3 - k + 1

                @pl.when(row_in(hub_row + k))
                def _():
                    pltpu.make_async_copy(ref.at[side], ref.at[side], seam_recv.at[i]).wait()

        fill(SEAM, [pack(ref[0], ref[1], None, None) for ref in (seam_up, seam_mid, seam_down)])
        inner = rows_in & (lane >= 32 - EDGE) & (lane < 32 + EDGE)
        seam_mask = row_mask_of(hub_row, FULL)
        seam = interleave((3 * k, sweep(k, [SEAM], FULL, seam_mask, None, lambda t, lane: inner)) for k in range(ITERS))
        seam_out[...] = xs[ITERS, SEAM, BASE + TOP : BASE + TOP + TR, :] * (1.0 / DSTEP)
        msg[...] = msg[...] + line_of(seam)
        back(2 * Y - 1).start()
        back(2 * Y).start()
        send_sums()

    for here, lanes, cols in (
        (before, lane32 >= 128 - EDGE, slice(TC - 128, TC)), (after, lane32 < EDGE, slice(0, 128))
    ):

        @pl.when(here)
        def _():
            pltpu.make_async_copy(seam_in, seam_in, back_recv).wait()
            out[:, cols] = jnp.where(lanes, pltpu.roll(seam_in[...], 96, 1), out[:, cols])

    def rows_of(ref, n, sem):
        return pltpu.make_async_copy(ref.at[0:n], ref.at[0:n], sem)

    for dr, dc in SIDES:
        pl.when(exists(dr, dc))(lambda dr=dr, dc=dc: halo(dr, dc).wait_send())
    for side, here in enumerate((before, after)):
        for k in (-1, 0, 1):
            pl.when(here & row_in(row + k))(lambda side=side, k=k: to_hub(side, k).wait_send())

    @pl.when(hub)
    def _():
        back(2 * Y - 1).wait_send()
        back(2 * Y).wait_send()

    pl.when(is_root)(lambda: rows_of(part, N_ROOTS - 1, part_send).wait())
    pl.when(jnp.logical_not(is_root))(lambda: rows_of(part, N_ROOTS, part_send).wait())

    @pl.when(is_root)
    def _():
        part[pl.ds(slot, 1), :] = msg[...]
        rows_of(part, N_ROW * N_COL - 1, part_recv).wait()
        total = [part[8 * i : 8 * i + 8] for i in range(N_ROW * N_COL // 8)]
        while len(total) > 1:
            total = [p + q for p, q in zip(total[::2], total[1::2])]
        total = jnp.sum(total[0], axis=0, keepdims=True)
        result[...] = total * (1.0 / (CELLS * DSTEP))

        def tell(target):
            pltpu.make_async_remote_copy(
                result, result, result_send, result_recv, device_id=target, device_id_type=pl.DeviceIdType.LOGICAL
            ).start()

        gap[...] = result[...]

        def tell_planes(start, stop):
            @pl.loop(start, stop)
            def _(zz):
                r, c = lax.rem(zz, Z_LO) * X + x, ((zz // Z_LO) * Y + y) * 2
                tell(ident(r, c))
                tell(ident(r, c + 1))

            rows_of(part, 2 * (stop - start), result_send).wait()

        pl.when(hub & (core == 0))(lambda: tell_planes(ALONE + 1, Z))

        @pl.when(hub & (core == 1) & jnp.logical_not(origin))
        def _():
            tell(ident(row, col - 1))
            tell_planes(1, Z)
            rows_of(part, 1, result_send).wait()


    @pl.when(jnp.logical_not(is_root))
    def _():
        pltpu.make_async_copy(result, result, result_recv).wait()
        gap[...] = result[...]


def finish(denoised, line, out, gap):
    out[...] = denoised[...]
    gap[...] = line[0, :ITERS]


def on_device(noisy):
    f32 = jnp.float32
    vmem = pl.BlockSpec(memory_space=pltpu.VMEM)
    frame = lambda n: pltpu.VMEM((n, NT + 2, BUF, 128), f32)
    dma = pltpu.SemaphoreType.DMA
    denoised, gap = pl.pallas_call(
        kernel,
        out_shape=(jax.ShapeDtypeStruct((TR, TC), f32), jax.ShapeDtypeStruct((1, 128), f32)),
        in_specs=[pl.BlockSpec(memory_space=pltpu.HBM)],
        out_specs=(vmem, vmem),
        scratch_shapes=[
            pltpu.VMEM((TR, TC), f32),
            pltpu.VMEM((8, TC), f32),
            pltpu.VMEM((8, TC), f32),
            pltpu.VMEM((TR, 128), f32),
            pltpu.VMEM((TR, 128), f32),
            pltpu.VMEM((4, 8, 128), f32),
            pltpu.VMEM((2, TR, 128), f32),
            pltpu.VMEM((2, 8, 128), f32),
            pltpu.VMEM((2, 8, 128), f32),
            pltpu.VMEM((TR, 128), f32),
            pltpu.VMEM((TR, 128), f32),
            frame(ITERS + 1), frame(1), frame(ITERS), frame(ITERS), frame(ITERS), frame(ITERS), frame(ITERS), frame(ITERS),
            pltpu.VMEM((1, 128), f32),
            pltpu.VMEM((N_ROW * N_COL, 128), f32),
            pltpu.VMEM((1, 128), f32),
            dma((4,)), dma((8,)), dma((8,)), dma, dma, dma, dma, dma((3,)), dma((6,)), dma((2,)), dma,
        ],
        compiler_params=pltpu.CompilerParams(
            collective_id=0, has_side_effects=True, vmem_limit_bytes=24 * 1024 * 1024
        ),
    )(pltpu.with_memory_space_constraint(noisy, pltpu.HBM))
    return pl.pallas_call(
        finish,
        out_shape=(jax.ShapeDtypeStruct((TR, TC), f32), jax.ShapeDtypeStruct((ITERS,), f32)),
        in_specs=[vmem, vmem],
        out_specs=(vmem, vmem),
        compiler_params=pltpu.CompilerParams(vmem_limit_bytes=4 * 1024 * 1024),
    )(denoised, gap)


def solution(mesh):
    return jax.shard_map(
        on_device,
        mesh=mesh,
        in_specs=(P("row", "col"),),
        out_specs=(P("row", "col"), P()),
        check_vma=False,
    )
```
